128 devices in a mesh: gx: 8 (over z, core), gy: 16 (over x, y).
Axes of the slice: x: 4, y: 4, z: 4, core: 2. Of those that a mesh axis runs over, the one named last changes fastest.
Arguments:
- prolong: bfloat16 [8192, 24, 128], P(('gx', 'gy')), may hold values from -0.5 to 0.5
- stiffness: bfloat16 [16384, 4, 128, 128], P(('gx', 'gy')), may hold values from -6 to 6
- request: int32 [16384], P(('gx', 'gy')), may hold values from 0 to 63, as said below
- col_slot: int32 [16384, 4], P(('gx', 'gy')), may hold values from 0 to 127
- col_pos: int32 [16384, 4], P(('gx', 'gy')), may hold values from 0 to 15, as said below
- coarse_owner: int32 [8192, 1], P(('gx', 'gy')), may hold values from 0 to 127; in each aligned block of 64 rows (0 to 63, 64 to 127, ...) no two rows name the same one
Outputs:
- coarse: float32 [16384, 24, 384], P(('gx', 'gy'))
The draws below stay inside these ranges and needn't reach their ends.
Inputs may be any that keep to these rules, and one draw needn't show every extreme that they name: `request`: on each device, entries k * 1 to (k + 1) * 1 - 1 name distinct aggregates of device k, as local indices there. `col_pos`: the 4 entries of one block row are distinct. `coarse_owner`: among one device's 64 aggregates at most 1 share a coarse owner, and on some devices 1 do.
All inputs are finite; a program needn't handle non-finite values.
Results may differ from the reference program's by a relative error of at most 0.0003.
Values may be sent and summed in bfloat16 or wider, within the bound.
A program may use at most 128 MiB of HBM per device.

```python
import math
import jax
import jax.numpy as jnp
import numpy as np
from jax import lax

AGG_DEV = 64
DOF = 128
CV = 24
MAXNB = 16
SLOT_DEV = 128
BPS = 4
SEND_MAX = 1
IN_ROWS = 128
NAGG = 8192
SLOTS = 16384
DEVICES = 128


def draw_request(key, part):
    per_peer = SLOT_DEV // DEVICES
    scores = jax.random.randint(key, (DEVICES * DEVICES, AGG_DEV), 0, 1 << 20) * AGG_DEV
    scores = scores + jnp.arange(AGG_DEV, dtype=jnp.int32)[None, :]
    chosen = jnp.argsort(scores, axis=1)[:, :per_peer]
    return chosen.reshape(-1).astype(jnp.int32)


def draw_col_pos(key, part):
    scores = jax.random.randint(key, (DEVICES * SLOT_DEV, MAXNB), 0, 1 << 20) * MAXNB
    scores = scores + jnp.arange(MAXNB, dtype=jnp.int32)[None, :]
    chosen = jnp.argsort(scores, axis=1)[:, :BPS]
    return chosen.astype(jnp.int32)


def touch_ends(values, key, low, high):
    longest = values.shape.index(max(values.shape))
    spots = []
    for shift in (0, 1):
        where = [jax.random.randint(jax.random.fold_in(key, axis), (), 0, length) for axis, length in enumerate(values.shape)]
        where[longest] = (where[longest] + shift) % values.shape[longest]
        spots.append(tuple(where))
    return values.at[spots[0]].set(low).at[spots[1]].set(high)


def level_of(own_key, shape, cuts, low, high):
    def one(position, shards_of):
        draws = jax.random.uniform(jax.random.fold_in(jax.random.fold_in(own_key, 6), position), (shards_of,), jnp.float32, low / len(cuts), high / len(cuts))
        return jnp.repeat(jnp.exp(draws), shape[position] // shards_of).reshape((-1,) + (1,) * (len(shape) - position - 1))

    factor_of = one(*cuts[0])
    for cut in cuts[1:]:
        factor_of = factor_of * one(*cut)
    return factor_of


def deal_out(stream_key, own, number, rows, count, top, reach, lean):
    order = jax.random.permutation(stream_key, count)
    heavy_load, common = load_shares(count, rows * top, reach, lean, True), load_shares(count, rows * top, reach, lean, False)
    places = jnp.arange(count)

    def named(sizes, offset_by):
        used = int((sizes > 0).sum())
        fixed = max(1, used // 4)
        shifted = fixed + (places - fixed + offset_by * (used - fixed)) % max(1, count - fixed)
        return jnp.zeros((count,), jnp.int32).at[order[jnp.where(places < fixed, places, shifted)]].set(jnp.asarray(sizes, jnp.int32))

    sizes = jnp.where(number % 4 == 0, named(heavy_load, number // 4), named(common, number - number // 4 - 1))
    mixed = jax.random.permutation(jax.random.fold_in(own, 3), count)
    source_of, taker = mixed[0:count // 2 * 2:2], mixed[1:count // 2 * 2:2]
    room = jnp.minimum(sizes[source_of] - 1, reach - sizes[taker]) // 2
    room = jnp.where((source_of == order[0]) | (taker == order[0]) | (sizes[taker] == 0), 0, jnp.maximum(room, 0))
    shifted = jax.random.randint(jax.random.fold_in(own, 4), (count // 2,), 0, 1 << 20) % (room + 1)
    sizes = sizes.at[source_of].add(-shifted).at[taker].add(shifted)
    items = jnp.searchsorted(jnp.cumsum(sizes), jnp.arange(rows * top), side="right").astype(jnp.int32)
    listing = items.reshape(top, rows).T
    listing = listing[jax.random.permutation(jax.random.fold_in(own, 1), rows)]
    offset_by = jax.random.randint(jax.random.fold_in(own, 2), (rows, 1), 0, top)
    return jnp.take_along_axis(listing, (jnp.arange(top)[None, :] + offset_by) % top, axis=1)


def load_shares(count, total, reach, slope, full):
    portions = [(1 << 20) // math.isqrt(rank ** slope) + 1 for rank in range(1, count + 1)]
    largest = reach if full else min(reach, max(-(-total // count), total * portions[0] // sum(portions)))
    least = 1 if total - largest >= count - 1 else 0
    holding, rest = [largest] + [least] * (count - 1), total - largest - least * (count - 1)
    while rest > 0:
        candidates = [i for i in range(1, count) if holding[i] < largest] or [i for i in range(1, count) if holding[i] < reach]
        whole, budget = sum([portions[i] for i in candidates]), rest
        for i in candidates:
            addition = min(reach - holding[i], max(1, budget * portions[i] // whole), rest)
            holding[i] = holding[i] + addition
            rest = rest - addition
    return np.array(holding)


def bell_draw(own_key, extent, width, limit, shards=(), held_as=jnp.bfloat16):
    values = width * jax.random.normal(own_key, extent, jnp.float32)
    if shards:
        values = values * level_of(own_key, extent, shards, -0.22, 0.18)
    return jnp.clip(values, -limit, limit).astype(held_as)


def setup_inputs(seed: int = 0) -> dict:
    arg_keys = jax.random.split(jax.random.key(seed), 7)
    prolong = bell_draw(arg_keys[0], (NAGG, CV, DOF), DOF ** -0.5, 0.5, ((0, 128),))
    stiffness = bell_draw(arg_keys[1], (SLOTS, BPS, DOF, DOF), 1.0, 6.0, ((0, 128),))
    request = draw_request(jax.random.fold_in(arg_keys[6], 71), 0)
    col_slot = touch_ends(jax.random.randint(arg_keys[3], (SLOTS, BPS), 0, SLOT_DEV), jax.random.fold_in(arg_keys[3], 1), 0, SLOT_DEV - 1).astype(jnp.int32)
    col_pos = draw_col_pos(jax.random.fold_in(arg_keys[6], 71), 0)
    coarse_owner_keys = jax.random.split(jax.random.fold_in(arg_keys[5], 1), NAGG // AGG_DEV)
    coarse_owner_turns = jax.random.permutation(jax.random.fold_in(arg_keys[5], 3), NAGG // AGG_DEV)
    coarse_owner = jax.vmap(lambda own, number: deal_out(jax.random.fold_in(arg_keys[5], 2), own, number, AGG_DEV, DEVICES, 1, SEND_MAX, 2))(coarse_owner_keys, coarse_owner_turns).reshape((NAGG, 1))
    return {"prolong": prolong, "stiffness": stiffness, "request": request, "col_slot": col_slot, "col_pos": col_pos, "coarse_owner": coarse_owner}


HIGH = lax.Precision.HIGHEST


def device_rows(prolong, stiff_block, request_block, slot_block, pos_block):
    per_peer = SLOT_DEV // DEVICES
    gid = (jnp.arange(SLOT_DEV, dtype=jnp.int32) // per_peer) * AGG_DEV + request_block.astype(jnp.int32)
    fetched = prolong[gid].astype(jnp.float32)
    col_rows = fetched[slot_block]
    applied = jnp.einsum("tqij,tqej->tqei", stiff_block.astype(jnp.float32), col_rows, precision=HIGH)
    partial_value = jnp.einsum("tci,tqei->tqce", fetched, applied, precision=HIGH)
    column_hot = (pos_block[:, :, None] == jnp.arange(MAXNB, dtype=jnp.int32)[None, None, :]).astype(jnp.float32)
    spread = jnp.einsum("tqce,tqn->tcne", partial_value, column_hot, precision=HIGH)
    return gid, spread.reshape(SLOT_DEV, CV, MAXNB * CV)


def reference(prolong, stiffness, request, col_slot, col_pos, coarse_owner):
    stiff_dev = stiffness.reshape(DEVICES, SLOT_DEV, BPS, DOF, DOF)
    request_dev = request.reshape(DEVICES, SLOT_DEV)
    slot_dev = col_slot.reshape(DEVICES, SLOT_DEV, BPS)
    pos_dev = col_pos.reshape(DEVICES, SLOT_DEV, BPS)

    def accumulate(total, pieces):
        gid, spread = device_rows(prolong, pieces[0], pieces[1], pieces[2], pieces[3])
        return total.at[gid].add(spread), None

    start = jnp.zeros((NAGG, CV, MAXNB * CV), jnp.float32)
    fine_coarse, _ = lax.scan(accumulate, start, (stiff_dev, request_dev, slot_dev, pos_dev))
    owners = coarse_owner[:, 0].reshape(DEVICES, AGG_DEV)
    peer_ids = jnp.arange(DEVICES, dtype=jnp.int32)
    owner_one = (owners[:, :, None] == peer_ids[None, None, :]).astype(jnp.int32)
    before = jnp.cumsum(owner_one, axis=1) - owner_one
    row_rank = jnp.sum(before * owner_one, axis=2)
    source = jnp.arange(DEVICES, dtype=jnp.int32)[:, None]
    target = (owners * IN_ROWS + source * SEND_MAX + row_rank).reshape(-1).astype(jnp.int32)
    coarse = jnp.zeros((DEVICES * IN_ROWS, CV, MAXNB * CV), jnp.float32).at[target].set(fine_coarse)
    return coarse
```

```python
import functools

import jax
import jax.numpy as jnp
from jax import lax
from jax.experimental import pallas as pl
from jax.experimental.pallas import tpu as pltpu
from jax.sharding import PartitionSpec as P

MESH = pl.DeviceIdType.MESH
STRIDE = 37
LEVELS = 32766.0
FLOOR = 1e-30
CHUNK = 16


def neighbour(s, gx, gy):
    o = lax.rem(s * STRIDE, 128)
    z, core, x, y = gx // 2, gx % 2, gy // 4, gy % 4
    z = (z + o // 32) % 4
    core = (core + (o // 16) % 2) % 2
    x = (x + (o // 4) % 4) % 4
    y = (y + o % 4) % 4
    tx, ty = z * 2 + core, x * 4 + y
    return {"gx": tx, "gy": ty}, tx * 16 + ty


def wait_all(ref, rows, sem):
    part = ref.at[pl.ds(0, rows)]
    pltpu.make_async_copy(part, part, sem).wait()


def exchange_kernel(
    request, slot_of, pos_of, owner_b, prolong, stiffness,
    arrived, scales,
    kbuf, ask, asked, asked_s, stage, fetched_in, fetched, payload, partial_in,
    plan, plan_s, running, outgoing, outscale,
    ksem, local, send, recv,
):
    devices = 128
    gx, gy = lax.axis_index("gx"), lax.axis_index("gy")
    me = gx * 16 + gy
    rows, width = payload.shape[1], payload.shape[2]
    cols = outgoing.shape[2]

    kcopies = [
        pltpu.make_async_copy(
            stiffness.at[pl.ds(c * CHUNK, CHUNK)], kbuf.at[pl.ds(c * CHUNK, CHUNK)], ksem.at[c]
        )
        for c in range(devices // CHUNK)
    ]
    for copy in kcopies:
        copy.start()

    barrier = pltpu.get_barrier_semaphore()

    @pl.loop(1, devices)
    def _(s):
        there, _ = neighbour(s, gx, gy)
        pl.semaphore_signal(barrier, inc=1, device_id=there, device_id_type=MESH)

    lane1 = lax.broadcasted_iota(jnp.int32, (1, 128), 1)

    @pl.loop(0, devices)
    def _(t):
        row = jnp.where(lane1 == 0, request[t], 0)
        for q in range(4):
            row = jnp.where(lane1 == q + 1, pos_of[q, t], row)
        ask[t] = row

    pl.semaphore_wait(barrier, devices - 1)

    def exchange(source, target, phase, lo=1, hi=devices):
        @pl.loop(lo, hi)
        def _(s):
            there, t = neighbour(s, gx, gy)
            pltpu.make_async_remote_copy(
                src_ref=source.at[t],
                dst_ref=target.at[me],
                send_sem=send.at[phase],
                recv_sem=recv.at[phase],
                device_id=there,
                device_id_type=MESH,
            ).start()

    def keep(source, target):
        copy = pltpu.make_async_copy(source.at[me], target.at[me], local)
        copy.start()
        copy.wait()

    exchange(ask, asked, 0)
    keep(ask, asked)
    wait_all(asked, devices - 1, recv.at[0])
    to_scalars = pltpu.make_async_copy(asked, asked_s, local)
    to_scalars.start()
    to_scalars.wait()

    @pl.loop(0, devices, unroll=4)
    def _(d):
        stage[d] = prolong[asked_s[d, 0, 0]]

    exchange(stage, fetched_in, 1)
    keep(stage, fetched_in)

    table = asked[...].reshape(devices, 128)
    wanted = jnp.transpose(table)[0:1, :]
    agg = lax.broadcasted_iota(jnp.int32, owner_b.shape, 0)
    goes_to = jnp.sum(jnp.where(agg == wanted, owner_b[...], 0), axis=0, keepdims=True)
    lane = lax.broadcasted_iota(jnp.int32, (devices, 128), 1)
    sub = lax.broadcasted_iota(jnp.int32, (devices, 128), 0)
    key_lane = jnp.broadcast_to(goes_to * 128 + lane1, (devices, 128))
    key_sub = jnp.transpose(key_lane)
    rank = jnp.sum((key_sub < key_lane).astype(jnp.int32), axis=0, keepdims=True)
    rank_sub = jnp.transpose(jnp.broadcast_to(rank, (devices, 128)))
    owner_sub = key_sub // 128
    here = rank_sub == lane
    order = jnp.sum(jnp.where(here, sub, 0), axis=0, keepdims=True)
    sorted_owner = jnp.sum(jnp.where(here, owner_sub, 0), axis=0, keepdims=True)
    before = pltpu.roll(sorted_owner, 1, 1)
    same = jnp.where(lane1 == 0, 0, (sorted_owner == before).astype(jnp.int32))
    up_to = jnp.sum((owner_sub <= lane).astype(jnp.int32), axis=0, keepdims=True)
    count = jnp.sum((owner_sub == lane).astype(jnp.int32), axis=0, keepdims=True)
    plan[0:1, :] = order
    plan[1:2, :] = same
    plan[2:3, :] = jnp.maximum(up_to - 1, 0)
    plan[3:4, :] = jnp.minimum(count, 1)
    to_scalars = pltpu.make_async_copy(plan, plan_s, local)
    to_scalars.start()
    to_scalars.wait()

    wait_all(fetched_in, devices - 1, recv.at[1])

    @pl.loop(0, devices, unroll=4)
    def _(t):
        fetched[t] = fetched_in[t].astype(jnp.float32)

    for copy in kcopies:
        copy.wait()

    lane_p = lax.broadcasted_iota(jnp.int32, (rows, width), 1)

    def triple(s):
        _, t = neighbour(s, gx, gy)
        p = fetched[t].astype(jnp.bfloat16)
        pieces, columns = [], []
        for q in range(4):
            pk = jnp.dot(p, kbuf[t, q], preferred_element_type=jnp.float32)
            high = pk.astype(jnp.bfloat16).astype(jnp.float32)
            pieces += [high, pk - high]
            columns.append(fetched[slot_of[q, t]])
        left = jnp.concatenate(pieces, axis=0).astype(jnp.bfloat16)
        right = jnp.concatenate(columns + [jnp.zeros((32, 128), jnp.float32)], axis=0).astype(jnp.bfloat16)
        both = lax.dot_general(
            left, right, (((1,), (1,)), ((), ())), preferred_element_type=jnp.float32
        )
        value = jnp.zeros((rows, width), jnp.float32)
        for q in range(4):
            mine = both[2 * q * rows : (2 * q + 1) * rows] + both[(2 * q + 1) * rows : (2 * q + 2) * rows]
            value = jnp.where((lane_p >= 24 * q) & (lane_p < 24 * (q + 1)), mine, value)
        top = jnp.maximum(jnp.max(jnp.abs(value), axis=1, keepdims=True), FLOOR)
        power = jnp.floor(jnp.log2(top)) + 1.0
        coded = jnp.clip(jnp.round(value * jnp.exp2(15.0 - power)), -32767.0, 32767.0)
        coded = jnp.where(lane_p >= 96, power, coded)
        payload[t] = coded.astype(jnp.int32).astype(jnp.int16)

    for c in range(devices // CHUNK):
        @pl.loop(c * CHUNK, (c + 1) * CHUNK, unroll=4)
        def _(s):
            triple(s)

        if c:
            exchange(payload, partial_in, 2, max(1, (c - 1) * CHUNK), c * CHUNK)
    exchange(payload, partial_in, 2, devices - CHUNK, devices)
    keep(payload, partial_in)
    wait_all(partial_in, devices - 1, recv.at[2])

    lanes = [lax.broadcasted_iota(jnp.int32, (rows, 128), 1) + 128 * j for j in range(cols // 128)]
    column = [l // 24 for l in lanes]
    within = [l % 24 for l in lanes]

    def add(i, carry):
        d = plan_s[0, i]
        joined = plan_s[1, i].astype(jnp.float32)
        got = partial_in[d].astype(jnp.int32).astype(jnp.float32)
        scale = jnp.exp2(got[:, 96:97] - 15.0)
        value = got * scale
        result = []
        for j in range(cols // 128):
            index = jnp.zeros((rows, 128), jnp.int32)
            hit = jnp.zeros((rows, 128), jnp.bool_)
            for q in range(4):
                eq = column[j] == asked_s[d, 0, q + 1]
                index = jnp.where(eq, within[j] + 24 * q, index)
                hit = hit | eq
            moved = jnp.take_along_axis(value, index, axis=1)
            total = carry[j] * joined + jnp.where(hit, moved, 0.0)
            running[i, :, 128 * j : 128 * (j + 1)] = total
            result.append(total)
        return tuple(result)

    zero = jnp.zeros((rows, 128), jnp.float32)
    lax.fori_loop(0, devices, add, (zero,) * (cols // 128), unroll=2)

    diagonal = lax.broadcasted_iota(jnp.int32, (rows, 128), 1) == lax.broadcasted_iota(
        jnp.int32, (rows, 128), 0
    )

    def encode(s):
        _, t = neighbour(s, gx, gy)
        value = running[plan_s[2, t]] * plan_s[3, t].astype(jnp.float32)
        top = jnp.maximum(jnp.max(jnp.abs(value), axis=1, keepdims=True), FLOOR)
        coded = jnp.round(value * (LEVELS / top))
        outgoing[t] = coded.astype(jnp.int32).astype(jnp.int16)
        outscale[t] = jnp.sum(jnp.where(diagonal, top * (1.0 / LEVELS), 0.0), axis=0, keepdims=True)

    for c in range(devices // CHUNK):
        @pl.loop(c * CHUNK, (c + 1) * CHUNK, unroll=2)
        def _(s):
            encode(s)

        if c:
            exchange(outgoing, arrived, 3, max(1, (c - 1) * CHUNK), c * CHUNK)
    exchange(outgoing, arrived, 3, devices - CHUNK, devices)
    exchange(outscale, scales, 4)
    keep(outgoing, arrived)
    keep(outscale, scales)

    wait_all(ask, devices - 1, send.at[0])
    wait_all(stage, devices - 1, send.at[1])
    wait_all(payload, devices - 1, send.at[2])
    wait_all(outgoing, devices - 1, send.at[3])
    wait_all(outscale, devices - 1, send.at[4])
    wait_all(arrived, devices - 1, recv.at[3])
    wait_all(scales, devices - 1, recv.at[4])


def decode_kernel(arrived, scales, out):
    rows, cols = out.shape[1], out.shape[2]
    diagonal = lax.broadcasted_iota(jnp.int32, (rows, 128), 1) == lax.broadcasted_iota(
        jnp.int32, (rows, 128), 0
    )

    @pl.loop(0, out.shape[0], unroll=4)
    def _(i):
        scale = jnp.sum(jnp.where(diagonal, scales[i], 0.0), axis=1, keepdims=True)
        out[i] = arrived[i].astype(jnp.int32).astype(jnp.float32) * scale


def per_device(prolong, stiffness, request, col_slot, col_pos, coarse_owner):
    slots, per_row, dof, _ = stiffness.shape
    vectors = prolong.shape[1]
    cols = 16 * vectors
    vmem = pl.BlockSpec(memory_space=pltpu.VMEM)
    smem = pl.BlockSpec(memory_space=pltpu.SMEM)
    owner_b = jnp.broadcast_to(coarse_owner, (coarse_owner.shape[0], 128))
    arrived, scales = pl.pallas_call(
        exchange_kernel,
        out_shape=(
            jax.ShapeDtypeStruct((slots, vectors, cols), jnp.int16),
            jax.ShapeDtypeStruct((slots, 1, 128), jnp.float32),
        ),
        in_specs=[smem, smem, smem, vmem, vmem, pl.BlockSpec(memory_space=pl.ANY)],
        out_specs=(vmem, vmem),
        scratch_shapes=[
            pltpu.VMEM((slots, per_row, dof, dof), jnp.bfloat16),
            pltpu.VMEM((slots, 1, 128), jnp.int32),
            pltpu.VMEM((slots, 1, 128), jnp.int32),
            pltpu.SMEM((slots, 1, 128), jnp.int32),
            pltpu.VMEM((slots, vectors, dof), jnp.bfloat16),
            pltpu.VMEM((slots, vectors, dof), jnp.bfloat16),
            pltpu.VMEM((slots, vectors, dof), jnp.float32),
            pltpu.VMEM((slots, vectors, 128), jnp.int16),
            pltpu.VMEM((slots, vectors, 128), jnp.int16),
            pltpu.VMEM((8, 128), jnp.int32),
            pltpu.SMEM((8, 128), jnp.int32),
            pltpu.VMEM((slots, vectors, cols), jnp.float32),
            pltpu.VMEM((slots, vectors, cols), jnp.int16),
            pltpu.VMEM((slots, 1, 128), jnp.float32),
            pltpu.SemaphoreType.DMA((slots // CHUNK,)),
            pltpu.SemaphoreType.DMA,
            pltpu.SemaphoreType.DMA((5,)),
            pltpu.SemaphoreType.DMA((5,)),
        ],
        compiler_params=pltpu.CompilerParams(
            collective_id=0, has_side_effects=True, vmem_limit_bytes=60 * 1024 * 1024
        ),
        name="galerkin_exchange",
    )(request, col_slot.T, col_pos.T, owner_b, prolong, stiffness)
    step = CHUNK
    return pl.pallas_call(
        decode_kernel,
        out_shape=jax.ShapeDtypeStruct((slots, vectors, cols), jnp.float32),
        grid=(slots // step,),
        in_specs=[
            pl.BlockSpec((step, vectors, cols), lambda i: (i, 0, 0)),
            pl.BlockSpec((step, 1, 128), lambda i: (i, 0, 0)),
        ],
        out_specs=pl.BlockSpec((step, vectors, cols), lambda i: (i, 0, 0)),
        name="decode",
    )(arrived, scales)


def solution(mesh):
    placed = (
        P(("gx", "gy"), None, None),
        P(("gx", "gy"), None, None, None),
        P(("gx", "gy")),
        P(("gx", "gy"), None),
        P(("gx", "gy"), None),
        P(("gx", "gy"), None),
    )
    return jax.shard_map(
        per_device,
        mesh=mesh,
        in_specs=placed,
        out_specs=P(("gx", "gy"), None, None),
        check_vma=False,
    )
```

```python
import jax
import jax.numpy as jnp
from jax import lax
from jax.experimental import pallas as pl
from jax.experimental.pallas import tpu as pltpu
from jax.sharding import PartitionSpec as P

MESH = pl.DeviceIdType.MESH
DEVICES = 128
STRIDE = 37
LEVELS = 32766.0
FLOOR = 1e-30
GROUP = 16
LAG = 2
TOP, LOW = 0b1011010, 0b0100101


def plus(me, s):
    o = (s * STRIDE) & (DEVICES - 1)
    return ((me & LOW) + (o & LOW)) ^ ((me ^ o) & TOP)


def minus(me, s):
    o = (s * STRIDE) & (DEVICES - 1)
    return ((me | TOP) - (o & LOW)) ^ ((me ^ ~o) & TOP)


def there(t):
    return {"gx": t >> 4, "gy": t & 15}


def wait_rows(ref, rows, sem):
    part = ref.at[pl.ds(0, rows)]
    pltpu.make_async_copy(part, part, sem).wait()


def exchange_kernel(
    request, slot_of, pos_of, owner_row, prolong, stiffness,
    arrived, scales,
    kbuf, ask, asked, table, table_s, stage, fetched_in, fetched, firsts, payload, partial_in,
    plan, plan_s, running, outgoing, outscale,
    ksem, local, send, recv, recv_block,
):
    me = lax.axis_index("gx") * 16 + lax.axis_index("gy")
    rows, width = payload.shape[1], payload.shape[2]
    cols = outgoing.shape[2]
    others = DEVICES - 1

    kcopy = pltpu.make_async_copy(stiffness, kbuf, ksem)
    kcopy.start()

    barrier = pltpu.get_barrier_semaphore()

    @pl.loop(1, DEVICES)
    def _(s):
        pl.semaphore_signal(barrier, inc=1, device_id=there(plus(me, s)), device_id_type=MESH)

    lane1 = lax.broadcasted_iota(jnp.int32, (1, 128), 1)

    @pl.loop(0, DEVICES, unroll=4)
    def _(t):
        row = jnp.where(lane1 == 0, request[t], 0)
        for q in range(4):
            row = jnp.where(lane1 == q + 1, pos_of[q, t], row)
        ask[t] = row

    pl.semaphore_wait(barrier, others)

    def push(source, target, t, send_sem, recv_sem):
        pltpu.make_async_remote_copy(
            src_ref=source.at[t],
            dst_ref=target.at[me],
            send_sem=send_sem,
            recv_sem=recv_sem,
            device_id=there(t),
            device_id_type=MESH,
        ).start()

    def keep(source, target, sem):
        pltpu.make_async_copy(source.at[me], target.at[me], sem).start()

    @pl.loop(1, DEVICES)
    def _(s):
        push(ask, asked, plus(me, s), send.at[0], recv.at[0])

    keep(ask, asked, recv.at[0])
    wait_rows(asked, DEVICES, recv.at[0])
    asks = jnp.transpose(asked[...].reshape(DEVICES, 128))
    table[...] = asks[0:8, :]
    to_scalars = pltpu.make_async_copy(table, table_s, local.at[0])
    to_scalars.start()
    to_scalars.wait()

    @pl.loop(0, DEVICES, unroll=8)
    def _(d):
        stage[d] = prolong[table_s[0, d]]

    @pl.loop(1, DEVICES)
    def _(s):
        push(stage, fetched_in, plus(me, s), send.at[1], recv_block.at[(s - 1) >> 4])

    keep(stage, fetched_in, recv_block.at[DEVICES // GROUP - 1])

    wanted = asks[0:1, :]
    own = jnp.transpose(jnp.broadcast_to(owner_row[...], (128, owner_row.shape[1])))
    agg = lax.broadcasted_iota(jnp.int32, own.shape, 0)
    goes_to = jnp.sum(jnp.where(agg == wanted, own, 0), axis=0, keepdims=True)
    lane = lax.broadcasted_iota(jnp.int32, (DEVICES, 128), 1)
    sub = lax.broadcasted_iota(jnp.int32, (DEVICES, 128), 0)
    key_lane = jnp.broadcast_to(goes_to * 128 + lane1, (DEVICES, 128))
    key_sub = jnp.transpose(key_lane)
    rank = jnp.sum((key_sub < key_lane).astype(jnp.int32), axis=0, keepdims=True)
    rank_sub = jnp.transpose(jnp.broadcast_to(rank, (DEVICES, 128)))
    owner_sub = key_sub >> 7
    here = rank_sub == lane
    order = jnp.sum(jnp.where(here, sub, 0), axis=0, keepdims=True)
    sorted_owner = jnp.sum(jnp.where(here, owner_sub, 0), axis=0, keepdims=True)
    before = pltpu.roll(sorted_owner, 1, 1)
    same = jnp.where(lane1 == 0, 0, (sorted_owner == before).astype(jnp.int32))
    up_to = jnp.sum((owner_sub <= lane).astype(jnp.int32), axis=0, keepdims=True)
    count = jnp.sum((owner_sub == lane).astype(jnp.int32), axis=0, keepdims=True)
    plan[0:1, :] = order
    plan[1:2, :] = same
    plan[2:3, :] = jnp.maximum(up_to - 1, 0)
    plan[3:4, :] = jnp.minimum(count, 1)
    plan_copy = pltpu.make_async_copy(plan, plan_s, local.at[1])
    plan_copy.start()

    kcopy.wait()

    @pl.loop(0, DEVICES // GROUP)
    def _(g):
        wait_rows(fetched_in, GROUP, recv_block.at[g])

        @pl.loop(0, GROUP, unroll=4)
        def _(i):
            t = minus(me, g * GROUP + i + 1)
            p = fetched_in[t]
            fetched[t] = p.astype(jnp.float32)
            pieces = []
            for q in range(4):
                pk = jnp.dot(p, kbuf[t, q], preferred_element_type=jnp.float32)
                high = pk.astype(jnp.bfloat16).astype(jnp.float32)
                pieces += [high, pk - high]
            firsts[t] = jnp.concatenate(pieces, axis=0).astype(jnp.bfloat16)

    lane_p = lax.broadcasted_iota(jnp.int32, (rows, width), 1)

    def second(s):
        t = plus(me, s)
        columns = [fetched[slot_of[q, t]] for q in range(4)]
        right = jnp.concatenate(columns + [jnp.zeros((32, 128), jnp.float32)], axis=0).astype(jnp.bfloat16)
        both = lax.dot_general(
            firsts[t], right, (((1,), (1,)), ((), ())), preferred_element_type=jnp.float32
        )
        value = jnp.zeros((rows, width), jnp.float32)
        for q in range(4):
            mine = both[2 * q * rows : (2 * q + 1) * rows] + both[(2 * q + 1) * rows : (2 * q + 2) * rows]
            value = jnp.where((lane_p >= 24 * q) & (lane_p < 24 * (q + 1)), mine, value)
        top = jnp.maximum(jnp.max(jnp.abs(value), axis=1, keepdims=True), FLOOR)
        power = jnp.floor(jnp.log2(top)) + 1.0
        coded = jnp.round(value * (jnp.exp2(-power) * LEVELS))
        coded = jnp.where(lane_p >= 96, power, coded)
        payload[t] = coded.astype(jnp.int32).astype(jnp.int16)

    def pipelined(make, post):
        @pl.loop(0, LAG)
        def _(g):
            for j in range(4):
                make(4 * g + j + 1)

        @pl.loop(LAG, DEVICES // 4)
        def _(g):
            for j in range(4):
                make(4 * g + j + 1)
            for j in range(4):
                post(4 * (g - LAG) + j + 1)

        @pl.loop(4 * (DEVICES // 4 - LAG) + 1, DEVICES)
        def _(s):
            post(s)

    pipelined(second, lambda s: push(payload, partial_in, plus(me, s), send.at[2], recv.at[1]))
    keep(payload, partial_in, recv.at[1])
    plan_copy.wait()
    wait_rows(partial_in, DEVICES, recv.at[1])

    lanes = [lax.broadcasted_iota(jnp.int32, (rows, 128), 1) + 128 * j for j in range(cols // 128)]
    column = [l // 24 for l in lanes]
    within = [l % 24 for l in lanes]
    blocks = cols // 128

    def spread(i):
        d = plan_s[0, i]
        got = partial_in[d].astype(jnp.int32).astype(jnp.float32)
        value = got * (jnp.exp2(got[:, 96:97]) * (1.0 / LEVELS))
        result = []
        for j in range(blocks):
            index = jnp.zeros((rows, 128), jnp.int32)
            hit = jnp.zeros((rows, 128), jnp.bool_)
            for q in range(4):
                eq = column[j] == table_s[q + 1, d]
                index = jnp.where(eq, within[j] + 24 * q, index)
                hit = hit | eq
            moved = jnp.take_along_axis(value, index, axis=1)
            result.append(jnp.where(hit, moved, 0.0))
        return result

    def add(g, carry):
        terms = [spread(4 * g + u) for u in range(4)]
        for u in range(4):
            joined = plan_s[1, 4 * g + u].astype(jnp.float32)
            carry = tuple(c * joined + v for c, v in zip(carry, terms[u]))
            for j in range(blocks):
                running[4 * g + u, :, 128 * j : 128 * (j + 1)] = carry[j]
        return carry

    zero = jnp.zeros((rows, 128), jnp.float32)
    lax.fori_loop(0, DEVICES // 4, add, (zero,) * blocks)

    diagonal = lax.broadcasted_iota(jnp.int32, (rows, 128), 1) == lax.broadcasted_iota(
        jnp.int32, (rows, 128), 0
    )

    def encode(s):
        t = plus(me, s)
        value = running[plan_s[2, t]] * plan_s[3, t].astype(jnp.float32)
        top = jnp.maximum(jnp.max(jnp.abs(value), axis=1, keepdims=True), FLOOR)
        coded = jnp.round(value * (LEVELS / top))
        outgoing[t] = coded.astype(jnp.int32).astype(jnp.int16)
        outscale[t] = jnp.sum(jnp.where(diagonal, top * (1.0 / LEVELS), 0.0), axis=0, keepdims=True)

    def post(s):
        t = plus(me, s)
        push(outscale, scales, t, send.at[4], recv.at[3])
        push(outgoing, arrived, t, send.at[3], recv.at[2])

    pipelined(encode, post)
    keep(outgoing, arrived, recv.at[2])
    keep(outscale, scales, recv.at[3])

    wait_rows(ask, others, send.at[0])
    wait_rows(stage, others, send.at[1])
    wait_rows(payload, others, send.at[2])
    wait_rows(outgoing, others, send.at[3])
    wait_rows(outscale, others, send.at[4])
    wait_rows(arrived, DEVICES, recv.at[2])
    wait_rows(scales, DEVICES, recv.at[3])


def decode_kernel(arrived, scales, out):
    rows = out.shape[1]
    diagonal = lax.broadcasted_iota(jnp.int32, (rows, 128), 1) == lax.broadcasted_iota(
        jnp.int32, (rows, 128), 0
    )

    @pl.loop(0, out.shape[0], unroll=4)
    def _(i):
        scale = jnp.sum(jnp.where(diagonal, scales[i], 0.0), axis=1, keepdims=True)
        out[i] = arrived[i].astype(jnp.int32).astype(jnp.float32) * scale


def per_device(prolong, stiffness, request, col_slot, col_pos, coarse_owner):
    slots, per_row, dof, _ = stiffness.shape
    vectors = prolong.shape[1]
    cols = 16 * vectors
    vmem = pl.BlockSpec(memory_space=pltpu.VMEM)
    smem = pl.BlockSpec(memory_space=pltpu.SMEM)
    arrived, scales = pl.pallas_call(
        exchange_kernel,
        out_shape=(
            jax.ShapeDtypeStruct((slots, vectors, cols), jnp.int16),
            jax.ShapeDtypeStruct((slots, 1, 128), jnp.float32),
        ),
        in_specs=[smem, smem, smem, vmem, vmem, pl.BlockSpec(memory_space=pl.ANY)],
        out_specs=(vmem, vmem),
        scratch_shapes=[
            pltpu.VMEM((slots, per_row, dof, dof), jnp.bfloat16),
            pltpu.VMEM((slots, 1, 128), jnp.int32),
            pltpu.VMEM((slots, 1, 128), jnp.int32),
            pltpu.VMEM((8, 128), jnp.int32),
            pltpu.SMEM((8, 128), jnp.int32),
            pltpu.VMEM((slots, vectors, dof), jnp.bfloat16),
            pltpu.VMEM((slots, vectors, dof), jnp.bfloat16),
            pltpu.VMEM((slots, vectors, dof), jnp.float32),
            pltpu.VMEM((slots, 2 * per_row * vectors, dof), jnp.bfloat16),
            pltpu.VMEM((slots, vectors, 128), jnp.int16),
            pltpu.VMEM((slots, vectors, 128), jnp.int16),
            pltpu.VMEM((8, 128), jnp.int32),
            pltpu.SMEM((8, 128), jnp.int32),
            pltpu.VMEM((slots, vectors, cols), jnp.float32),
            pltpu.VMEM((slots, vectors, cols), jnp.int16),
            pltpu.VMEM((slots, 1, 128), jnp.float32),
            pltpu.SemaphoreType.DMA,
            pltpu.SemaphoreType.DMA((2,)),
            pltpu.SemaphoreType.DMA((5,)),
            pltpu.SemaphoreType.DMA((4,)),
            pltpu.SemaphoreType.DMA((slots // GROUP,)),
        ],
        compiler_params=pltpu.CompilerParams(
            collective_id=0, has_side_effects=True, vmem_limit_bytes=60 * 1024 * 1024
        ),
        name="galerkin_exchange",
    )(request, col_slot.T, col_pos.T, coarse_owner.T, prolong, stiffness)
    step = GROUP
    return pl.pallas_call(
        decode_kernel,
        out_shape=jax.ShapeDtypeStruct((slots, vectors, cols), jnp.float32),
        grid=(slots // step,),
        in_specs=[
            pl.BlockSpec((step, vectors, cols), lambda i: (i, 0, 0)),
            pl.BlockSpec((step, 1, 128), lambda i: (i, 0, 0)),
        ],
        out_specs=pl.BlockSpec((step, vectors, cols), lambda i: (i, 0, 0)),
        name="decode",
    )(arrived, scales)


def solution(mesh):
    placed = (
        P(("gx", "gy"), None, None),
        P(("gx", "gy"), None, None, None),
        P(("gx", "gy")),
        P(("gx", "gy"), None),
        P(("gx", "gy"), None),
        P(("gx", "gy"), None),
    )
    return jax.shard_map(
        per_device,
        mesh=mesh,
        in_specs=placed,
        out_specs=P(("gx", "gy"), None, None),
        check_vma=False,
    )
```

```python
import jax
import jax.numpy as jnp
from jax import lax
from jax.experimental import pallas as pl
from jax.experimental.pallas import tpu as pltpu
from jax.sharding import PartitionSpec as P

MESH = pl.DeviceIdType.MESH
DEVICES = 128
STRIDE = 37
LEVELS = 32766.0
FLOOR = 1e-30
GROUP = 16
LAG = 2
TOP, LOW = 0b1011010, 0b0100101


def plus(me, o):
    return ((me & LOW) + (o & LOW)) ^ ((me ^ o) & TOP)


def minus(me, o):
    return ((me | TOP) - (o & LOW)) ^ ((me ^ ~o) & TOP)


def mixed(s):
    return (s * STRIDE) & (DEVICES - 1)


def hops(o):
    return sum(min(d, 4 - d) for d in (o >> 5, (o >> 2) & 3, o & 3))


BY_HOPS = sorted((mixed(s) for s in range(1, DEVICES)), key=lambda o: -hops(o))


def there(t):
    return {"gx": t >> 4, "gy": t & 15}


def wait_rows(ref, rows, sem):
    part = ref.at[pl.ds(0, rows)]
    pltpu.make_async_copy(part, part, sem).wait()


def exchange_kernel(
    request_in, slot_in, pos_in, owner_in, prolong_in, stiffness,
    arrived, scales,
    request, slot_of, pos_of, owner_row, prolong,
    kbuf, ask, asked, table, table_s, stage, fetched_in, fetched, firsts, payload, partial_in,
    plan, plan_s, spread, running, outgoing, outscale,
    ksem, load, local, send, recv, recv_block, recv_row,
):
    me = lax.axis_index("gx") * 16 + lax.axis_index("gy")
    rows, width = payload.shape[1], payload.shape[2]
    cols = outgoing.shape[2]
    others = DEVICES - 1

    loads = [
        pltpu.make_async_copy(source, target, load.at[k])
        for k, (source, target) in enumerate(
            ((request_in, request), (pos_in, pos_of), (slot_in, slot_of), (owner_in, owner_row), (prolong_in, prolong))
        )
    ]
    for copy in loads:
        copy.start()
    kcopy = pltpu.make_async_copy(stiffness, kbuf, ksem)
    kcopy.start()

    barrier = pltpu.get_barrier_semaphore()
    for o in BY_HOPS:
        pl.semaphore_signal(barrier, inc=1, device_id=there(plus(me, o)), device_id_type=MESH)
    for copy in loads:
        copy.wait()

    lane1 = lax.broadcasted_iota(jnp.int32, (1, 128), 1)

    @pl.loop(0, DEVICES, unroll=4)
    def _(t):
        row = jnp.where(lane1 == 0, request[t], 0)
        for q in range(4):
            row = jnp.where(lane1 == q + 1, pos_of[q, t], row)
        ask[t] = row

    pl.semaphore_wait(barrier, others)

    def push(source, target, t, send_sem, recv_sem):
        pltpu.make_async_remote_copy(
            src_ref=source.at[t],
            dst_ref=target.at[me],
            send_sem=send_sem,
            recv_sem=recv_sem,
            device_id=there(t),
            device_id_type=MESH,
        ).start()

    def keep(source, target, sem):
        pltpu.make_async_copy(source.at[me], target.at[me], sem).start()

    for o in BY_HOPS:
        push(ask, asked, plus(me, o), send.at[0], recv.at[0])

    keep(ask, asked, recv.at[0])
    wait_rows(asked, DEVICES, recv.at[0])
    asks = jnp.transpose(asked[...].reshape(DEVICES, 128))
    table[...] = asks[0:8, :]
    to_scalars = pltpu.make_async_copy(table, table_s, local.at[0])
    to_scalars.start()
    to_scalars.wait()

    @pl.loop(0, DEVICES, unroll=8)
    def _(d):
        stage[d] = prolong[table_s[0, d]]

    for s in range(1, DEVICES):
        push(stage, fetched_in, plus(me, mixed(s)), send.at[1], recv_block.at[(s - 1) // GROUP])

    keep(stage, fetched_in, recv_block.at[DEVICES // GROUP - 1])

    wanted = asks[0:1, :]
    own = jnp.transpose(jnp.broadcast_to(owner_row[...], (128, owner_row.shape[1])))
    agg = lax.broadcasted_iota(jnp.int32, own.shape, 0)
    goes_to = jnp.sum(jnp.where(agg == wanted, own, 0), axis=0, keepdims=True)
    lane = lax.broadcasted_iota(jnp.int32, (DEVICES, 128), 1)
    sub = lax.broadcasted_iota(jnp.int32, (DEVICES, 128), 0)
    key_lane = jnp.broadcast_to(goes_to * 128 + lane1, (DEVICES, 128))
    key_sub = jnp.transpose(key_lane)
    rank = jnp.sum((key_sub < key_lane).astype(jnp.int32), axis=0, keepdims=True)
    rank_sub = jnp.transpose(jnp.broadcast_to(rank, (DEVICES, 128)))
    owner_sub = key_sub >> 7
    here = rank_sub == lane
    order = jnp.sum(jnp.where(here, sub, 0), axis=0, keepdims=True)
    sorted_owner = jnp.sum(jnp.where(here, owner_sub, 0), axis=0, keepdims=True)
    before = pltpu.roll(sorted_owner, 1, 1)
    same = jnp.where(lane1 == 0, 0, (sorted_owner == before).astype(jnp.int32))
    up_to = jnp.sum((owner_sub <= lane).astype(jnp.int32), axis=0, keepdims=True)
    count = jnp.sum((owner_sub == lane).astype(jnp.int32), axis=0, keepdims=True)
    plan[0:1, :] = order
    plan[1:2, :] = same
    plan[2:3, :] = jnp.maximum(up_to - 1, 0)
    plan[3:4, :] = jnp.minimum(count, 1)
    plan_copy = pltpu.make_async_copy(plan, plan_s, local.at[1])
    plan_copy.start()

    kcopy.wait()

    @pl.loop(0, DEVICES // GROUP)
    def _(g):
        wait_rows(fetched_in, GROUP, recv_block.at[g])

        @pl.loop(0, GROUP, unroll=4)
        def _(i):
            t = minus(me, mixed(g * GROUP + i + 1))
            p = fetched_in[t]
            fetched[t] = p.astype(jnp.float32)
            pieces = []
            for q in range(4):
                pk = jnp.dot(p, kbuf[t, q], preferred_element_type=jnp.float32)
                high = pk.astype(jnp.bfloat16).astype(jnp.float32)
                pieces += [high, pk - high]
            firsts[t] = jnp.concatenate(pieces, axis=0).astype(jnp.bfloat16)

    lane_p = lax.broadcasted_iota(jnp.int32, (rows, width), 1)

    def second(s):
        t = plus(me, mixed(s))
        columns = [fetched[slot_of[q, t]] for q in range(4)]
        right = jnp.concatenate(columns + [jnp.zeros((32, 128), jnp.float32)], axis=0).astype(jnp.bfloat16)
        both = lax.dot_general(
            firsts[t], right, (((1,), (1,)), ((), ())), preferred_element_type=jnp.float32
        )
        value = jnp.zeros((rows, width), jnp.float32)
        for q in range(4):
            mine = both[2 * q * rows : (2 * q + 1) * rows] + both[(2 * q + 1) * rows : (2 * q + 2) * rows]
            value = jnp.where((lane_p >= 24 * q) & (lane_p < 24 * (q + 1)), mine, value)
        top = jnp.maximum(jnp.max(jnp.abs(value), axis=1, keepdims=True), FLOOR)
        power = jnp.floor(jnp.log2(top)) + 1.0
        coded = jnp.round(value * (jnp.exp2(-power) * LEVELS))
        coded = jnp.where(lane_p >= 96, power, coded)
        payload[t] = coded.astype(jnp.int32).astype(jnp.int16)

    def pipelined(make, post):
        @pl.loop(0, LAG)
        def _(g):
            for j in range(4):
                make(4 * g + j + 1)

        @pl.loop(LAG, DEVICES // 4)
        def _(g):
            for j in range(4):
                make(4 * g + j + 1)
            for j in range(4):
                post(4 * (g - LAG) + j + 1)

        @pl.loop(4 * (DEVICES // 4 - LAG) + 1, DEVICES)
        def _(s):
            post(s)

    pipelined(
        second,
        lambda s: push(
            payload, partial_in, plus(me, mixed(s)), send.at[2], recv_row.at[(s - 1) >> 4]
        ),
    )
    keep(payload, partial_in, recv_row.at[DEVICES // GROUP - 1])

    lanes = [lax.broadcasted_iota(jnp.int32, (rows, 128), 1) + 128 * j for j in range(cols // 128)]
    column = [l // 24 for l in lanes]
    within = [l % 24 for l in lanes]
    blocks = cols // 128

    def place(d):
        got = partial_in[d].astype(jnp.int32).astype(jnp.float32)
        value = got * (jnp.exp2(got[:, 96:97]) * (1.0 / LEVELS))
        for j in range(blocks):
            index = jnp.zeros((rows, 128), jnp.int32)
            hit = jnp.zeros((rows, 128), jnp.bool_)
            for q in range(4):
                eq = column[j] == table_s[q + 1, d]
                index = jnp.where(eq, within[j] + 24 * q, index)
                hit = hit | eq
            moved = jnp.take_along_axis(value, index, axis=1)
            spread[d, :, 128 * j : 128 * (j + 1)] = jnp.where(hit, moved, 0.0)

    @pl.loop(0, DEVICES // GROUP)
    def _(g):
        wait_rows(partial_in, GROUP, recv_row.at[g])

        @pl.loop(0, GROUP // 4)
        def _(i):
            for u in range(4):
                place(minus(me, mixed(g * GROUP + 4 * i + u + 1)))

    plan_copy.wait()

    def add(g, carry):
        terms = [spread[plan_s[0, 4 * g + u]] for u in range(4)]
        for u in range(4):
            joined = plan_s[1, 4 * g + u].astype(jnp.float32)
            carry = carry * joined + terms[u]
            running[4 * g + u] = carry
        return carry

    lax.fori_loop(0, DEVICES // 4, add, jnp.zeros((rows, cols), jnp.float32))

    diagonal = lax.broadcasted_iota(jnp.int32, (rows, 128), 1) == lax.broadcasted_iota(
        jnp.int32, (rows, 128), 0
    )

    def encode(s):
        t = plus(me, mixed(s))
        value = running[plan_s[2, t]] * plan_s[3, t].astype(jnp.float32)
        top = jnp.maximum(jnp.max(jnp.abs(value), axis=1, keepdims=True), FLOOR)
        coded = jnp.round(value * (LEVELS / top))
        outgoing[t] = coded.astype(jnp.int32).astype(jnp.int16)
        outscale[t] = jnp.sum(jnp.where(diagonal, top * (1.0 / LEVELS), 0.0), axis=0, keepdims=True)

    def post(s):
        t = plus(me, mixed(s))
        push(outscale, scales, t, send.at[4], recv.at[2])
        push(outgoing, arrived, t, send.at[3], recv.at[1])

    pipelined(encode, post)
    keep(outgoing, arrived, recv.at[1])
    keep(outscale, scales, recv.at[2])

    wait_rows(ask, others, send.at[0])
    wait_rows(stage, others, send.at[1])
    wait_rows(payload, others, send.at[2])
    wait_rows(outgoing, others, send.at[3])
    wait_rows(outscale, others, send.at[4])
    wait_rows(arrived, DEVICES, recv.at[1])
    wait_rows(scales, DEVICES, recv.at[2])


def decode_kernel(arrived, scales_in, out, codes, scales, values, in_sem, scale_sem, out_sem):
    rows = values.shape[1]
    diagonal = lax.broadcasted_iota(jnp.int32, (rows, 128), 1) == lax.broadcasted_iota(
        jnp.int32, (rows, 128), 0
    )

    def copies(source, target, sem):
        return [
            pltpu.make_async_copy(source.at[pl.ds(c * GROUP, GROUP)], target.at[pl.ds(c * GROUP, GROUP)], sem.at[c])
            for c in range(DEVICES // GROUP)
        ]

    reads, writes = copies(arrived, codes, in_sem), copies(values, out, out_sem)
    scale_read = pltpu.make_async_copy(scales_in, scales, scale_sem)
    scale_read.start()
    for copy in reads:
        copy.start()
    scale_read.wait()
    for c in range(DEVICES // GROUP):
        reads[c].wait()

        @pl.loop(c * GROUP, (c + 1) * GROUP, unroll=4)
        def _(i):
            scale = jnp.sum(jnp.where(diagonal, scales[i], 0.0), axis=1, keepdims=True)
            values[i] = codes[i].astype(jnp.int32).astype(jnp.float32) * scale

        writes[c].start()
    for copy in writes:
        copy.wait()


def per_device(prolong, stiffness, request, col_slot, col_pos, coarse_owner):
    slots, per_row, dof, _ = stiffness.shape
    vectors = prolong.shape[1]
    cols = 16 * vectors
    vmem = pl.BlockSpec(memory_space=pltpu.VMEM)
    hbm = pl.BlockSpec(memory_space=pl.ANY)
    arrived, scales = pl.pallas_call(
        exchange_kernel,
        out_shape=(
            jax.ShapeDtypeStruct((slots, vectors, cols), jnp.int16),
            jax.ShapeDtypeStruct((slots, 1, 128), jnp.float32),
        ),
        in_specs=[hbm] * 6,
        out_specs=(hbm, hbm),
        scratch_shapes=[
            pltpu.SMEM((slots,), jnp.int32),
            pltpu.SMEM((per_row, slots), jnp.int32),
            pltpu.SMEM((per_row, slots), jnp.int32),
            pltpu.VMEM((1, coarse_owner.shape[0]), jnp.int32),
            pltpu.VMEM(prolong.shape, jnp.bfloat16),
            pltpu.VMEM((slots, per_row, dof, dof), jnp.bfloat16),
            pltpu.VMEM((slots, 1, 128), jnp.int32),
            pltpu.VMEM((slots, 1, 128), jnp.int32),
            pltpu.VMEM((8, 128), jnp.int32),
            pltpu.SMEM((8, 128), jnp.int32),
            pltpu.VMEM((slots, vectors, dof), jnp.bfloat16),
            pltpu.VMEM((slots, vectors, dof), jnp.bfloat16),
            pltpu.VMEM((slots, vectors, dof), jnp.float32),
            pltpu.VMEM((slots, 2 * per_row * vectors, dof), jnp.bfloat16),
            pltpu.VMEM((slots, vectors, 128), jnp.int16),
            pltpu.VMEM((slots, vectors, 128), jnp.int16),
            pltpu.VMEM((8, 128), jnp.int32),
            pltpu.SMEM((8, 128), jnp.int32),
            pltpu.VMEM((slots, vectors, cols), jnp.float32),
            pltpu.VMEM((slots, vectors, cols), jnp.float32),
            pltpu.VMEM((slots, vectors, cols), jnp.int16),
            pltpu.VMEM((slots, 1, 128), jnp.float32),
            pltpu.SemaphoreType.DMA,
            pltpu.SemaphoreType.DMA((5,)),
            pltpu.SemaphoreType.DMA((2,)),
            pltpu.SemaphoreType.DMA((5,)),
            pltpu.SemaphoreType.DMA((3,)),
            pltpu.SemaphoreType.DMA((slots // GROUP,)),
            pltpu.SemaphoreType.DMA((slots // GROUP,)),
        ],
        compiler_params=pltpu.CompilerParams(
            collective_id=0, has_side_effects=True, vmem_limit_bytes=60 * 1024 * 1024
        ),
        name="galerkin_exchange",
    )(request, col_slot.T, col_pos.T, coarse_owner.T, prolong, stiffness)
    return pl.pallas_call(
        decode_kernel,
        out_shape=jax.ShapeDtypeStruct((slots, vectors, cols), jnp.float32),
        in_specs=[hbm, hbm],
        out_specs=hbm,
        scratch_shapes=[
            pltpu.VMEM((slots, vectors, cols), jnp.int16),
            pltpu.VMEM((slots, 1, 128), jnp.float32),
            pltpu.VMEM((slots, vectors, cols), jnp.float32),
            pltpu.SemaphoreType.DMA((slots // GROUP,)),
            pltpu.SemaphoreType.DMA,
            pltpu.SemaphoreType.DMA((slots // GROUP,)),
        ],
        compiler_params=pltpu.CompilerParams(vmem_limit_bytes=60 * 1024 * 1024),
        name="decode",
    )(arrived, scales)


def solution(mesh):
    placed = (
        P(("gx", "gy"), None, None),
        P(("gx", "gy"), None, None, None),
        P(("gx", "gy")),
        P(("gx", "gy"), None),
        P(("gx", "gy"), None),
        P(("gx", "gy"), None),
    )
    return jax.shard_map(
        per_device,
        mesh=mesh,
        in_specs=placed,
        out_specs=P(("gx", "gy"), None, None),
        check_vma=False,
    )
```

```python
import jax
import jax.numpy as jnp
from jax import lax
from jax.experimental import pallas as pl
from jax.experimental.pallas import tpu as pltpu
from jax.sharding import PartitionSpec as P

MESH = pl.DeviceIdType.MESH
DEVICES = 128
STRIDE = 37
LEVELS = 32766.0
FLOOR = 1e-30
GROUP = 16
STEPS = 8
LAG = 2
TOP, LOW = 0b1011010, 0b0100101


def plus(me, o):
    return ((me & LOW) + (o & LOW)) ^ ((me ^ o) & TOP)


def minus(me, o):
    return ((me | TOP) - (o & LOW)) ^ ((me ^ ~o) & TOP)


def mixed(s):
    return (s * STRIDE) & (DEVICES - 1)


def hops(o):
    return sum(min(d, 4 - d) for d in (o >> 5, (o >> 2) & 3, o & 3))


BY_HOPS = sorted((mixed(s) for s in range(1, DEVICES)), key=lambda o: -hops(o))


def there(t):
    return {"gx": t >> 4, "gy": t & 15}


def wait_rows(ref, rows, sem):
    part = ref.at[pl.ds(0, rows)]
    pltpu.make_async_copy(part, part, sem).wait()


def exchange_kernel(
    request_in, slot_in, pos_in, owner_in, prolong_in, stiffness,
    result,
    request, slot_of, pos_of, owner_row, prolong,
    kbuf, ask, asked, table, table_s, stage, fetched_in, fetched, firsts, payload, partial_in,
    plan, plan_s, spread, running, outgoing, arrived, outscale, scales,
    ksem, load, local, send, recv, recv_block, recv_row, recv_last, recv_scale,
):
    me = lax.axis_index("gx") * 16 + lax.axis_index("gy")
    rows, width = payload.shape[1], payload.shape[2]
    cols = outgoing.shape[2]
    others = DEVICES - 1

    loads = [
        pltpu.make_async_copy(source, target, load.at[k])
        for k, (source, target) in enumerate(
            ((request_in, request), (pos_in, pos_of), (slot_in, slot_of), (owner_in, owner_row), (prolong_in, prolong))
        )
    ]
    for copy in loads:
        copy.start()
    kcopy = pltpu.make_async_copy(stiffness, kbuf, ksem)
    kcopy.start()

    barrier = pltpu.get_barrier_semaphore()
    for o in BY_HOPS:
        pl.semaphore_signal(barrier, inc=1, device_id=there(plus(me, o)), device_id_type=MESH)
    for copy in loads:
        copy.wait()

    lane1 = lax.broadcasted_iota(jnp.int32, (1, 128), 1)

    @pl.loop(0, DEVICES, unroll=4)
    def _(t):
        row = jnp.where(lane1 == 0, request[t], 0)
        for q in range(4):
            row = jnp.where(lane1 == q + 1, pos_of[q, t], row)
        ask[t] = row

    pl.semaphore_wait(barrier, others)

    def push(source, target, t, send_sem, recv_sem):
        pltpu.make_async_remote_copy(
            src_ref=source.at[t],
            dst_ref=target.at[me],
            send_sem=send_sem,
            recv_sem=recv_sem,
            device_id=there(t),
            device_id_type=MESH,
        ).start()

    def keep(source, target, sem):
        pltpu.make_async_copy(source.at[me], target.at[me], sem).start()

    for o in BY_HOPS:
        push(ask, asked, plus(me, o), send.at[0], recv.at[0])

    keep(ask, asked, recv.at[0])
    wait_rows(asked, DEVICES, recv.at[0])
    asks = jnp.transpose(asked[...].reshape(DEVICES, 128))
    table[...] = asks[0:8, :]
    to_scalars = pltpu.make_async_copy(table, table_s, local.at[0])
    to_scalars.start()
    to_scalars.wait()

    @pl.loop(0, DEVICES, unroll=8)
    def _(d):
        stage[d] = prolong[table_s[0, d]]

    for s in range(1, DEVICES):
        push(stage, fetched_in, plus(me, mixed(s)), send.at[1], recv_block.at[(s - 1) // GROUP])

    keep(stage, fetched_in, recv_block.at[DEVICES // GROUP - 1])

    wanted = asks[0:1, :]
    own = jnp.transpose(jnp.broadcast_to(owner_row[...], (128, owner_row.shape[1])))
    agg = lax.broadcasted_iota(jnp.int32, own.shape, 0)
    goes_to = jnp.sum(jnp.where(agg == wanted, own, 0), axis=0, keepdims=True)
    lane = lax.broadcasted_iota(jnp.int32, (DEVICES, 128), 1)
    sub = lax.broadcasted_iota(jnp.int32, (DEVICES, 128), 0)
    key_lane = jnp.broadcast_to(goes_to * 128 + lane1, (DEVICES, 128))
    key_sub = jnp.transpose(key_lane)
    rank = jnp.sum((key_sub < key_lane).astype(jnp.int32), axis=0, keepdims=True)
    rank_sub = jnp.transpose(jnp.broadcast_to(rank, (DEVICES, 128)))
    owner_sub = key_sub >> 7
    here = rank_sub == lane
    order = jnp.sum(jnp.where(here, sub, 0), axis=0, keepdims=True)
    sorted_owner = jnp.sum(jnp.where(here, owner_sub, 0), axis=0, keepdims=True)
    before = pltpu.roll(sorted_owner, 1, 1)
    same = jnp.where(lane1 == 0, 0, (sorted_owner == before).astype(jnp.int32))
    up_to = jnp.sum((owner_sub <= lane).astype(jnp.int32), axis=0, keepdims=True)
    count = jnp.sum((owner_sub == lane).astype(jnp.int32), axis=0, keepdims=True)
    plan[0:1, :] = order
    plan[1:2, :] = same
    plan[2:3, :] = jnp.maximum(up_to - 1, 0)
    plan[3:4, :] = jnp.minimum(count, 1)
    plan_copy = pltpu.make_async_copy(plan, plan_s, local.at[1])
    plan_copy.start()

    kcopy.wait()

    @pl.loop(0, DEVICES // GROUP)
    def _(g):
        wait_rows(fetched_in, GROUP, recv_block.at[g])

        @pl.loop(0, GROUP, unroll=4)
        def _(i):
            t = minus(me, mixed(g * GROUP + i + 1))
            p = fetched_in[t]
            fetched[t] = p.astype(jnp.float32)
            pieces = []
            for q in range(4):
                pk = jnp.dot(p, kbuf[t, q], preferred_element_type=jnp.float32)
                high = pk.astype(jnp.bfloat16).astype(jnp.float32)
                pieces += [high, pk - high]
            firsts[t] = jnp.concatenate(pieces, axis=0).astype(jnp.bfloat16)

    lane_p = lax.broadcasted_iota(jnp.int32, (rows, width), 1)

    def second(s):
        t = plus(me, mixed(s))
        columns = [fetched[slot_of[q, t]] for q in range(4)]
        right = jnp.concatenate(columns + [jnp.zeros((32, 128), jnp.float32)], axis=0).astype(jnp.bfloat16)
        both = lax.dot_general(
            firsts[t], right, (((1,), (1,)), ((), ())), preferred_element_type=jnp.float32
        )
        value = jnp.zeros((rows, width), jnp.float32)
        for q in range(4):
            mine = both[2 * q * rows : (2 * q + 1) * rows] + both[(2 * q + 1) * rows : (2 * q + 2) * rows]
            value = jnp.where((lane_p >= 24 * q) & (lane_p < 24 * (q + 1)), mine, value)
        top = jnp.maximum(jnp.max(jnp.abs(value), axis=1, keepdims=True), FLOOR)
        step = jnp.ceil(jnp.log2(top) * STEPS)
        coded = jnp.round(value * (jnp.exp2(step * (-1.0 / STEPS)) * LEVELS))
        coded = jnp.where(lane_p >= 96, step, coded)
        payload[t] = coded.astype(jnp.int32).astype(jnp.int16)

    def pipelined(make, post):
        @pl.loop(0, LAG)
        def _(g):
            for j in range(4):
                make(4 * g + j + 1)

        @pl.loop(LAG, DEVICES // 4)
        def _(g):
            for j in range(4):
                make(4 * g + j + 1)
            for j in range(4):
                post(4 * (g - LAG) + j + 1)

        @pl.loop(4 * (DEVICES // 4 - LAG) + 1, DEVICES)
        def _(s):
            post(s)

    pipelined(
        second,
        lambda s: push(
            payload, partial_in, plus(me, mixed(s)), send.at[2], recv_row.at[(s - 1) >> 4]
        ),
    )
    keep(payload, partial_in, recv_row.at[DEVICES // GROUP - 1])

    lanes = [lax.broadcasted_iota(jnp.int32, (rows, 128), 1) + 128 * j for j in range(cols // 128)]
    column = [l // 24 for l in lanes]
    within = [l % 24 for l in lanes]
    blocks = cols // 128

    def place(d):
        got = partial_in[d].astype(jnp.int32).astype(jnp.float32)
        value = got * (jnp.exp2(got[:, 96:97] * (1.0 / STEPS)) * (1.0 / LEVELS))
        for j in range(blocks):
            index = jnp.zeros((rows, 128), jnp.int32)
            hit = jnp.zeros((rows, 128), jnp.bool_)
            for q in range(4):
                eq = column[j] == table_s[q + 1, d]
                index = jnp.where(eq, within[j] + 24 * q, index)
                hit = hit | eq
            moved = jnp.take_along_axis(value, index, axis=1)
            spread[d, :, 128 * j : 128 * (j + 1)] = jnp.where(hit, moved, 0.0)

    @pl.loop(0, DEVICES // GROUP)
    def _(g):
        wait_rows(partial_in, GROUP, recv_row.at[g])

        @pl.loop(0, GROUP // 4)
        def _(i):
            for u in range(4):
                place(minus(me, mixed(g * GROUP + 4 * i + u + 1)))

    plan_copy.wait()

    def add(g, carry):
        terms = [spread[plan_s[0, 4 * g + u]] for u in range(4)]
        for u in range(4):
            joined = plan_s[1, 4 * g + u].astype(jnp.float32)
            carry = carry * joined + terms[u]
            running[4 * g + u] = carry
        return carry

    lax.fori_loop(0, DEVICES // 4, add, jnp.zeros((rows, cols), jnp.float32))

    diagonal = lax.broadcasted_iota(jnp.int32, (rows, 128), 1) == lax.broadcasted_iota(
        jnp.int32, (rows, 128), 0
    )

    def encode(s):
        t = plus(me, mixed(s))
        value = running[plan_s[2, t]] * plan_s[3, t].astype(jnp.float32)
        top = jnp.maximum(jnp.max(jnp.abs(value), axis=1, keepdims=True), FLOOR)
        outgoing[t] = jnp.round(value * (LEVELS / top)).astype(jnp.int32).astype(jnp.int16)
        outscale[t] = jnp.sum(jnp.where(diagonal, top * (1.0 / LEVELS), 0.0), axis=0, keepdims=True)

    def post(s):
        t = plus(me, mixed(s))
        push(outscale, scales, t, send.at[4], recv_scale.at[(s - 1) >> 4])
        push(outgoing, arrived, t, send.at[3], recv_last.at[(s - 1) >> 4])

    pipelined(encode, post)
    keep(outscale, scales, recv_scale.at[DEVICES // GROUP - 1])
    keep(outgoing, arrived, recv_last.at[DEVICES // GROUP - 1])

    @pl.loop(0, DEVICES // GROUP)
    def _(g):
        wait_rows(scales, GROUP, recv_scale.at[g])
        wait_rows(arrived, GROUP, recv_last.at[g])

        @pl.loop(0, GROUP // 4)
        def _(i):
            for u in range(4):
                t = minus(me, mixed(g * GROUP + 4 * i + u + 1))
                scale = jnp.sum(jnp.where(diagonal, scales[t], 0.0), axis=1, keepdims=True)
                result[t] = arrived[t].astype(jnp.int32).astype(jnp.float32) * scale

    for k, ref in enumerate((ask, stage, payload, outgoing, outscale)):
        wait_rows(ref, others, send.at[k])


def store_kernel(values, out, sem):
    copies = [
        pltpu.make_async_copy(
            values.at[pl.ds(c * GROUP, GROUP)], out.at[pl.ds(c * GROUP, GROUP)], sem.at[c]
        )
        for c in range(DEVICES // GROUP)
    ]
    for copy in copies:
        copy.start()
    for copy in copies:
        copy.wait()


def per_device(prolong, stiffness, request, col_slot, col_pos, coarse_owner):
    slots, per_row, dof, _ = stiffness.shape
    vectors = prolong.shape[1]
    cols = 16 * vectors
    vmem = pl.BlockSpec(memory_space=pltpu.VMEM)
    hbm = pl.BlockSpec(memory_space=pl.ANY)
    result = pl.pallas_call(
        exchange_kernel,
        out_shape=pltpu.VMEM((slots, vectors, cols), jnp.float32),
        in_specs=[hbm] * 6,
        out_specs=vmem,
        scratch_shapes=[
            pltpu.SMEM((slots,), jnp.int32),
            pltpu.SMEM((per_row, slots), jnp.int32),
            pltpu.SMEM((per_row, slots), jnp.int32),
            pltpu.VMEM((1, coarse_owner.shape[0]), jnp.int32),
            pltpu.VMEM(prolong.shape, jnp.bfloat16),
            pltpu.VMEM((slots, per_row, dof, dof), jnp.bfloat16),
            pltpu.VMEM((slots, 1, 128), jnp.int32),
            pltpu.VMEM((slots, 1, 128), jnp.int32),
            pltpu.VMEM((8, 128), jnp.int32),
            pltpu.SMEM((8, 128), jnp.int32),
            pltpu.VMEM((slots, vectors, dof), jnp.bfloat16),
            pltpu.VMEM((slots, vectors, dof), jnp.bfloat16),
            pltpu.VMEM((slots, vectors, dof), jnp.float32),
            pltpu.VMEM((slots, 2 * per_row * vectors, dof), jnp.bfloat16),
            pltpu.VMEM((slots, vectors, 128), jnp.int16),
            pltpu.VMEM((slots, vectors, 128), jnp.int16),
            pltpu.VMEM((8, 128), jnp.int32),
            pltpu.SMEM((8, 128), jnp.int32),
            pltpu.VMEM((slots, vectors, cols), jnp.float32),
            pltpu.VMEM((slots, vectors, cols), jnp.float32),
            pltpu.VMEM((slots, vectors, cols), jnp.int16),
            pltpu.VMEM((slots, vectors, cols), jnp.int16),
            pltpu.VMEM((slots, 1, 128), jnp.float32),
            pltpu.VMEM((slots, 1, 128), jnp.float32),
            pltpu.SemaphoreType.DMA,
            pltpu.SemaphoreType.DMA((5,)),
            pltpu.SemaphoreType.DMA((2,)),
            pltpu.SemaphoreType.DMA((5,)),
            pltpu.SemaphoreType.DMA((1,)),
            pltpu.SemaphoreType.DMA((slots // GROUP,)),
            pltpu.SemaphoreType.DMA((slots // GROUP,)),
            pltpu.SemaphoreType.DMA((slots // GROUP,)),
            pltpu.SemaphoreType.DMA((slots // GROUP,)),
        ],
        compiler_params=pltpu.CompilerParams(
            collective_id=0, has_side_effects=True, vmem_limit_bytes=56 * 1024 * 1024
        ),
        name="galerkin_exchange",
    )(request, col_slot.T, col_pos.T, coarse_owner.T, prolong, stiffness)
    return pl.pallas_call(
        store_kernel,
        out_shape=jax.ShapeDtypeStruct((slots, vectors, cols), jnp.float32),
        in_specs=[vmem],
        out_specs=hbm,
        scratch_shapes=[pltpu.SemaphoreType.DMA((slots // GROUP,))],
        compiler_params=pltpu.CompilerParams(vmem_limit_bytes=16 * 1024 * 1024),
        name="store",
    )(result)


def solution(mesh):
    placed = (
        P(("gx", "gy"), None, None),
        P(("gx", "gy"), None, None, None),
        P(("gx", "gy")),
        P(("gx", "gy"), None),
        P(("gx", "gy"), None),
        P(("gx", "gy"), None),
    )
    return jax.shard_map(
        per_device,
        mesh=mesh,
        in_specs=placed,
        out_specs=P(("gx", "gy"), None, None),
        check_vma=False,
    )
```

```python
import jax
import jax.numpy as jnp
from jax import lax
from jax.experimental import pallas as pl
from jax.experimental.pallas import tpu as pltpu
from jax.sharding import PartitionSpec as P

MESH = pl.DeviceIdType.MESH
DEVICES = 128
STRIDE = 53
LEVELS = 32766.0
FLOOR = 1e-30
GROUP = 8
STEPS = 8
LAG = 1
TOP, LOW = 0b1011010, 0b0100101


def plus(me, o):
    return ((me & LOW) + (o & LOW)) ^ ((me ^ o) & TOP)


def minus(me, o):
    return ((me | TOP) - (o & LOW)) ^ ((me ^ ~o) & TOP)


def mixed(s):
    return (s * STRIDE) & (DEVICES - 1)


def hops(o):
    return sum(min(d, 4 - d) for d in (o >> 5, (o >> 2) & 3, o & 3))


BY_HOPS = sorted((mixed(s) for s in range(1, DEVICES)), key=lambda o: -hops(o))


def there(t):
    return {"gx": t >> 4, "gy": t & 15}


def wait_rows(ref, rows, sem):
    part = ref.at[pl.ds(0, rows)]
    pltpu.make_async_copy(part, part, sem).wait()


def exchange_kernel(
    request_in, slot_in, pos_in, owner_in, prolong_in, stiffness,
    result,
    request, slot_of, pos_of, owner_row, prolong,
    kbuf, ask, asked, table, table_s, stage, fetched_in, fetched, firsts, payload, partial_in,
    plan, plan_s, spread, running, outgoing, arrived, outscale, scales,
    ksem, load, local, send, recv, recv_block, recv_row, recv_last, recv_scale,
):
    me = lax.axis_index("gx") * 16 + lax.axis_index("gy")
    rows, width = payload.shape[1], payload.shape[2]
    cols = outgoing.shape[2]
    others = DEVICES - 1

    loads = [
        pltpu.make_async_copy(source, target, load.at[k])
        for k, (source, target) in enumerate(
            ((request_in, request), (pos_in, pos_of), (slot_in, slot_of), (owner_in, owner_row), (prolong_in, prolong))
        )
    ]
    for copy in loads:
        copy.start()
    kcopy = pltpu.make_async_copy(stiffness, kbuf, ksem)
    kcopy.start()

    barrier = pltpu.get_barrier_semaphore()
    for o in BY_HOPS:
        pl.semaphore_signal(barrier, inc=1, device_id=there(plus(me, o)), device_id_type=MESH)
    for copy in loads:
        copy.wait()

    lane1 = lax.broadcasted_iota(jnp.int32, (1, 128), 1)

    @pl.loop(0, DEVICES, unroll=4)
    def _(t):
        row = jnp.where(lane1 == 0, request[t], 0)
        for q in range(4):
            row = jnp.where(lane1 == q + 1, pos_of[q, t], row)
        ask[t] = row

    pl.semaphore_wait(barrier, others)

    def push(source, target, t, send_sem, recv_sem):
        pltpu.make_async_remote_copy(
            src_ref=source.at[t],
            dst_ref=target.at[me],
            send_sem=send_sem,
            recv_sem=recv_sem,
            device_id=there(t),
            device_id_type=MESH,
        ).start()

    def keep(source, target, sem):
        pltpu.make_async_copy(source.at[me], target.at[me], sem).start()

    for o in BY_HOPS:
        push(ask, asked, plus(me, o), send.at[0], recv.at[0])

    keep(ask, asked, recv.at[0])
    wait_rows(asked, DEVICES, recv.at[0])
    asks = jnp.transpose(asked[...].reshape(DEVICES, 128))
    table[...] = asks[0:8, :]
    to_scalars = pltpu.make_async_copy(table, table_s, local.at[0])
    to_scalars.start()
    to_scalars.wait()

    @pl.loop(0, DEVICES, unroll=8)
    def _(d):
        stage[d] = prolong[table_s[0, d]]

    for s in range(1, DEVICES):
        push(stage, fetched_in, plus(me, mixed(s)), send.at[1], recv_block.at[(s - 1) // GROUP])

    keep(stage, fetched_in, recv_block.at[DEVICES // GROUP - 1])

    wanted = asks[0:1, :]
    own = jnp.transpose(jnp.broadcast_to(owner_row[...], (128, owner_row.shape[1])))
    agg = lax.broadcasted_iota(jnp.int32, own.shape, 0)
    goes_to = jnp.sum(jnp.where(agg == wanted, own, 0), axis=0, keepdims=True)
    lane = lax.broadcasted_iota(jnp.int32, (DEVICES, 128), 1)
    sub = lax.broadcasted_iota(jnp.int32, (DEVICES, 128), 0)
    key_lane = jnp.broadcast_to(goes_to * 128 + lane1, (DEVICES, 128))
    key_sub = jnp.transpose(key_lane)
    rank = jnp.sum((key_sub < key_lane).astype(jnp.int32), axis=0, keepdims=True)
    rank_sub = jnp.transpose(jnp.broadcast_to(rank, (DEVICES, 128)))
    owner_sub = key_sub >> 7
    here = rank_sub == lane
    order = jnp.sum(jnp.where(here, sub, 0), axis=0, keepdims=True)
    sorted_owner = jnp.sum(jnp.where(here, owner_sub, 0), axis=0, keepdims=True)
    before = pltpu.roll(sorted_owner, 1, 1)
    same = jnp.where(lane1 == 0, 0, (sorted_owner == before).astype(jnp.int32))
    up_to = jnp.sum((owner_sub <= lane).astype(jnp.int32), axis=0, keepdims=True)
    count = jnp.sum((owner_sub == lane).astype(jnp.int32), axis=0, keepdims=True)
    plan[0:1, :] = order
    plan[1:2, :] = same
    plan[2:3, :] = jnp.maximum(up_to - 1, 0)
    plan[3:4, :] = jnp.minimum(count, 1)
    plan_copy = pltpu.make_async_copy(plan, plan_s, local.at[1])
    plan_copy.start()

    kcopy.wait()

    @pl.loop(0, DEVICES // GROUP)
    def _(g):
        wait_rows(fetched_in, GROUP, recv_block.at[g])

        @pl.loop(0, GROUP, unroll=4)
        def _(i):
            t = minus(me, mixed(g * GROUP + i + 1))
            p = fetched_in[t]
            fetched[t] = p.astype(jnp.float32)
            pieces = []
            for q in range(4):
                pk = jnp.dot(p, kbuf[t, q], preferred_element_type=jnp.float32)
                high = pk.astype(jnp.bfloat16).astype(jnp.float32)
                pieces += [high, pk - high]
            firsts[t] = jnp.concatenate(pieces, axis=0).astype(jnp.bfloat16)

    lane_p = lax.broadcasted_iota(jnp.int32, (rows, width), 1)

    def second(s):
        t = plus(me, mixed(s))
        columns = [fetched[slot_of[q, t]] for q in range(4)]
        right = jnp.concatenate(columns + [jnp.zeros((32, 128), jnp.float32)], axis=0).astype(jnp.bfloat16)
        both = lax.dot_general(
            firsts[t], right, (((1,), (1,)), ((), ())), preferred_element_type=jnp.float32
        )
        value = jnp.zeros((rows, width), jnp.float32)
        for q in range(4):
            mine = both[2 * q * rows : (2 * q + 1) * rows] + both[(2 * q + 1) * rows : (2 * q + 2) * rows]
            value = jnp.where((lane_p >= 24 * q) & (lane_p < 24 * (q + 1)), mine, value)
        top = jnp.maximum(jnp.max(jnp.abs(value), axis=1, keepdims=True), FLOOR)
        step = jnp.ceil(jnp.log2(top) * STEPS)
        coded = jnp.round(value * (jnp.exp2(step * (-1.0 / STEPS)) * LEVELS))
        coded = jnp.where(lane_p >= 96, step, coded)
        payload[t] = coded.astype(jnp.int32).astype(jnp.int16)

    def pipelined(make, post):
        @pl.loop(0, LAG)
        def _(g):
            for j in range(4):
                make(4 * g + j + 1)

        @pl.loop(LAG, DEVICES // 4)
        def _(g):
            for j in range(4):
                make(4 * g + j + 1)
            for j in range(4):
                post(4 * (g - LAG) + j + 1)

        @pl.loop(4 * (DEVICES // 4 - LAG) + 1, DEVICES)
        def _(s):
            post(s)

    pipelined(
        second,
        lambda s: push(
            payload, partial_in, plus(me, mixed(s)), send.at[2], recv_row.at[(s - 1) >> 3]
        ),
    )
    keep(payload, partial_in, recv_row.at[DEVICES // GROUP - 1])

    lanes = [lax.broadcasted_iota(jnp.int32, (rows, 128), 1) + 128 * j for j in range(cols // 128)]
    column = [l // 24 for l in lanes]
    within = [l % 24 for l in lanes]
    blocks = cols // 128

    def place(d):
        got = partial_in[d].astype(jnp.int32).astype(jnp.float32)
        value = got * (jnp.exp2(got[:, 96:97] * (1.0 / STEPS)) * (1.0 / LEVELS))
        for j in range(blocks):
            index = jnp.zeros((rows, 128), jnp.int32)
            hit = jnp.zeros((rows, 128), jnp.bool_)
            for q in range(4):
                eq = column[j] == table_s[q + 1, d]
                index = jnp.where(eq, within[j] + 24 * q, index)
                hit = hit | eq
            moved = jnp.take_along_axis(value, index, axis=1)
            spread[d, :, 128 * j : 128 * (j + 1)] = jnp.where(hit, moved, 0.0)

    @pl.loop(0, DEVICES // GROUP)
    def _(g):
        wait_rows(partial_in, GROUP, recv_row.at[g])

        @pl.loop(0, GROUP // 4)
        def _(i):
            for u in range(4):
                place(minus(me, mixed(g * GROUP + 4 * i + u + 1)))

    plan_copy.wait()

    def add(g, carry):
        terms = [spread[plan_s[0, 4 * g + u]] for u in range(4)]
        for u in range(4):
            joined = plan_s[1, 4 * g + u].astype(jnp.float32)
            carry = carry * joined + terms[u]
            running[4 * g + u] = carry
        return carry

    lax.fori_loop(0, DEVICES // 4, add, jnp.zeros((rows, cols), jnp.float32))

    diagonal = lax.broadcasted_iota(jnp.int32, (rows, 128), 1) == lax.broadcasted_iota(
        jnp.int32, (rows, 128), 0
    )

    def encode(s):
        t = plus(me, mixed(s))
        value = running[plan_s[2, t]] * plan_s[3, t].astype(jnp.float32)
        top = jnp.maximum(jnp.max(jnp.abs(value), axis=1, keepdims=True), FLOOR)
        outgoing[t] = jnp.round(value * (LEVELS / top)).astype(jnp.int32).astype(jnp.int16)
        outscale[t] = jnp.sum(jnp.where(diagonal, top * (1.0 / LEVELS), 0.0), axis=0, keepdims=True)

    def post(s):
        t = plus(me, mixed(s))
        push(outscale, scales, t, send.at[4], recv_scale.at[(s - 1) >> 3])
        push(outgoing, arrived, t, send.at[3], recv_last.at[(s - 1) >> 3])

    pipelined(encode, post)
    keep(outscale, scales, recv_scale.at[DEVICES // GROUP - 1])
    keep(outgoing, arrived, recv_last.at[DEVICES // GROUP - 1])

    @pl.loop(0, DEVICES // GROUP)
    def _(g):
        wait_rows(scales, GROUP, recv_scale.at[g])
        wait_rows(arrived, GROUP, recv_last.at[g])

        @pl.loop(0, GROUP // 4)
        def _(i):
            for u in range(4):
                t = minus(me, mixed(g * GROUP + 4 * i + u + 1))
                scale = jnp.sum(jnp.where(diagonal, scales[t], 0.0), axis=1, keepdims=True)
                result[t] = arrived[t].astype(jnp.int32).astype(jnp.float32) * scale

    for k, ref in enumerate((ask, stage, payload, outgoing, outscale)):
        wait_rows(ref, others, send.at[k])


def store_kernel(values, out, sem):
    copies = [
        pltpu.make_async_copy(
            values.at[pl.ds(c * GROUP, GROUP)], out.at[pl.ds(c * GROUP, GROUP)], sem.at[c]
        )
        for c in range(DEVICES // GROUP)
    ]
    for copy in copies:
        copy.start()
    for copy in copies:
        copy.wait()


def per_device(prolong, stiffness, request, col_slot, col_pos, coarse_owner):
    slots, per_row, dof, _ = stiffness.shape
    vectors = prolong.shape[1]
    cols = 16 * vectors
    vmem = pl.BlockSpec(memory_space=pltpu.VMEM)
    hbm = pl.BlockSpec(memory_space=pl.ANY)
    result = pl.pallas_call(
        exchange_kernel,
        out_shape=pltpu.VMEM((slots, vectors, cols), jnp.float32),
        in_specs=[hbm] * 6,
        out_specs=vmem,
        scratch_shapes=[
            pltpu.SMEM((slots,), jnp.int32),
            pltpu.SMEM((per_row, slots), jnp.int32),
            pltpu.SMEM((per_row, slots), jnp.int32),
            pltpu.VMEM((1, coarse_owner.shape[0]), jnp.int32),
            pltpu.VMEM(prolong.shape, jnp.bfloat16),
            pltpu.VMEM((slots, per_row, dof, dof), jnp.bfloat16),
            pltpu.VMEM((slots, 1, 128), jnp.int32),
            pltpu.VMEM((slots, 1, 128), jnp.int32),
            pltpu.VMEM((8, 128), jnp.int32),
            pltpu.SMEM((8, 128), jnp.int32),
            pltpu.VMEM((slots, vectors, dof), jnp.bfloat16),
            pltpu.VMEM((slots, vectors, dof), jnp.bfloat16),
            pltpu.VMEM((slots, vectors, dof), jnp.float32),
            pltpu.VMEM((slots, 2 * per_row * vectors, dof), jnp.bfloat16),
            pltpu.VMEM((slots, vectors, 128), jnp.int16),
            pltpu.VMEM((slots, vectors, 128), jnp.int16),
            pltpu.VMEM((8, 128), jnp.int32),
            pltpu.SMEM((8, 128), jnp.int32),
            pltpu.VMEM((slots, vectors, cols), jnp.float32),
            pltpu.VMEM((slots, vectors, cols), jnp.float32),
            pltpu.VMEM((slots, vectors, cols), jnp.int16),
            pltpu.VMEM((slots, vectors, cols), jnp.int16),
            pltpu.VMEM((slots, 1, 128), jnp.float32),
            pltpu.VMEM((slots, 1, 128), jnp.float32),
            pltpu.SemaphoreType.DMA,
            pltpu.SemaphoreType.DMA((5,)),
            pltpu.SemaphoreType.DMA((2,)),
            pltpu.SemaphoreType.DMA((5,)),
            pltpu.SemaphoreType.DMA((1,)),
            pltpu.SemaphoreType.DMA((slots // GROUP,)),
            pltpu.SemaphoreType.DMA((slots // GROUP,)),
            pltpu.SemaphoreType.DMA((slots // GROUP,)),
            pltpu.SemaphoreType.DMA((slots // GROUP,)),
        ],
        compiler_params=pltpu.CompilerParams(
            collective_id=0, has_side_effects=True, vmem_limit_bytes=56 * 1024 * 1024
        ),
        name="galerkin_exchange",
    )(request, col_slot.T, col_pos.T, coarse_owner.T, prolong, stiffness)
    return pl.pallas_call(
        store_kernel,
        out_shape=jax.ShapeDtypeStruct((slots, vectors, cols), jnp.float32),
        in_specs=[vmem],
        out_specs=hbm,
        scratch_shapes=[pltpu.SemaphoreType.DMA((slots // GROUP,))],
        compiler_params=pltpu.CompilerParams(vmem_limit_bytes=16 * 1024 * 1024),
        name="store",
    )(result)


def solution(mesh):
    placed = (
        P(("gx", "gy"), None, None),
        P(("gx", "gy"), None, None, None),
        P(("gx", "gy")),
        P(("gx", "gy"), None),
        P(("gx", "gy"), None),
        P(("gx", "gy"), None),
    )
    return jax.shard_map(
        per_device,
        mesh=mesh,
        in_specs=placed,
        out_specs=P(("gx", "gy"), None, None),
        check_vma=False,
    )
```

```python
import jax
import jax.numpy as jnp
from jax import lax
from jax.experimental import pallas as pl
from jax.experimental.pallas import tpu as pltpu
from jax.sharding import PartitionSpec as P

MESH = pl.DeviceIdType.MESH
DEVICES = 128
STRIDE = 53
LEVELS = 32766.0
FLOOR = 1e-30
GROUP = 8
STEPS = 8
LAG = 1
TOP, LOW = 0b1011010, 0b0100101


def plus(me, o):
    return ((me & LOW) + (o & LOW)) ^ ((me ^ o) & TOP)


def minus(me, o):
    return ((me | TOP) - (o & LOW)) ^ ((me ^ ~o) & TOP)


def mixed(s):
    return (s * STRIDE) & (DEVICES - 1)


def hops(o):
    return sum(min(d, 4 - d) for d in (o >> 5, (o >> 2) & 3, o & 3))


BY_HOPS = sorted((mixed(s) for s in range(1, DEVICES)), key=lambda o: -hops(o))


def there(t):
    return {"gx": t >> 4, "gy": t & 15}


def wait_rows(ref, rows, sem):
    part = ref.at[pl.ds(0, rows)]
    pltpu.make_async_copy(part, part, sem).wait()


def exchange_kernel(
    request_in, slot_in, pos_in, owner_in, prolong_in, stiffness,
    result,
    request, slot_of, pos_of, owner_row, prolong,
    kbuf, ask, asked, table, table_s, stage, fetched_in, fetched, firsts, payload, partial_in,
    plan, plan_s, spread, running, outgoing, arrived, outscale, scales,
    ksem, load, local, send, recv, recv_block, recv_row, recv_last, recv_scale,
):
    me = lax.axis_index("gx") * 16 + lax.axis_index("gy")
    rows, width = payload.shape[1], payload.shape[2]
    cols = outgoing.shape[2]
    others = DEVICES - 1

    loads = [
        pltpu.make_async_copy(source, target, load.at[k])
        for k, (source, target) in enumerate(
            ((request_in, request), (pos_in, pos_of), (slot_in, slot_of), (owner_in, owner_row), (prolong_in, prolong))
        )
    ]
    for copy in loads:
        copy.start()
    kcopy = pltpu.make_async_copy(stiffness, kbuf, ksem)
    kcopy.start()

    barrier = pltpu.get_barrier_semaphore()
    for o in BY_HOPS:
        pl.semaphore_signal(barrier, inc=1, device_id=there(plus(me, o)), device_id_type=MESH)
    for copy in loads:
        copy.wait()

    lane1 = lax.broadcasted_iota(jnp.int32, (1, 128), 1)

    @pl.loop(0, DEVICES, unroll=4)
    def _(t):
        row = jnp.where(lane1 == 0, request[t], 0)
        for q in range(4):
            row = jnp.where(lane1 == q + 1, pos_of[q, t], row)
        ask[t] = row

    pl.semaphore_wait(barrier, others)

    def push(source, target, t, send_sem, recv_sem):
        pltpu.make_async_remote_copy(
            src_ref=source.at[t],
            dst_ref=target.at[me],
            send_sem=send_sem,
            recv_sem=recv_sem,
            device_id=there(t),
            device_id_type=MESH,
        ).start()

    def keep(source, target, sem):
        pltpu.make_async_copy(source.at[me], target.at[me], sem).start()

    for o in BY_HOPS:
        push(ask, asked, plus(me, o), send.at[0], recv.at[0])

    keep(ask, asked, recv.at[0])
    wait_rows(asked, DEVICES, recv.at[0])
    asks = jnp.transpose(asked[...].reshape(DEVICES, 128))
    table[...] = asks[0:8, :]
    to_scalars = pltpu.make_async_copy(table, table_s, local.at[0])
    to_scalars.start()
    to_scalars.wait()

    @pl.loop(0, DEVICES, unroll=8)
    def _(d):
        stage[d] = prolong[table_s[0, d]]

    for s in range(1, DEVICES):
        push(stage, fetched_in, plus(me, mixed(s)), send.at[1], recv_block.at[(s - 1) // GROUP])

    keep(stage, fetched_in, recv_block.at[DEVICES // GROUP - 1])

    wanted = asks[0:1, :]
    own = jnp.transpose(jnp.broadcast_to(owner_row[...], (128, owner_row.shape[1])))
    agg = lax.broadcasted_iota(jnp.int32, own.shape, 0)
    goes_to = jnp.sum(jnp.where(agg == wanted, own, 0), axis=0, keepdims=True)
    lane = lax.broadcasted_iota(jnp.int32, (DEVICES, 128), 1)
    sub = lax.broadcasted_iota(jnp.int32, (DEVICES, 128), 0)
    key_lane = jnp.broadcast_to(goes_to * 128 + lane1, (DEVICES, 128))
    key_sub = jnp.transpose(key_lane)
    rank = jnp.sum((key_sub < key_lane).astype(jnp.int32), axis=0, keepdims=True)
    rank_sub = jnp.transpose(jnp.broadcast_to(rank, (DEVICES, 128)))
    owner_sub = key_sub >> 7
    here = rank_sub == lane
    order = jnp.sum(jnp.where(here, sub, 0), axis=0, keepdims=True)
    sorted_owner = jnp.sum(jnp.where(here, owner_sub, 0), axis=0, keepdims=True)
    before = pltpu.roll(sorted_owner, 1, 1)
    same = jnp.where(lane1 == 0, 0, (sorted_owner == before).astype(jnp.int32))
    up_to = jnp.sum((owner_sub <= lane).astype(jnp.int32), axis=0, keepdims=True)
    count = jnp.sum((owner_sub == lane).astype(jnp.int32), axis=0, keepdims=True)
    plan[0:1, :] = order
    plan[1:2, :] = same
    plan[2:3, :] = jnp.maximum(up_to - 1, 0)
    plan[3:4, :] = jnp.minimum(count, 1)
    plan_copy = pltpu.make_async_copy(plan, plan_s, local.at[1])
    plan_copy.start()

    kcopy.wait()

    @pl.loop(0, DEVICES // GROUP)
    def _(g):
        wait_rows(fetched_in, GROUP, recv_block.at[g])

        @pl.loop(0, GROUP, unroll=8)
        def _(i):
            t = minus(me, mixed(g * GROUP + i + 1))
            p = fetched_in[t]
            fetched[t] = p.astype(jnp.float32)
            pieces = []
            for q in range(4):
                pk = jnp.dot(p, kbuf[t, q], preferred_element_type=jnp.float32)
                high = pk.astype(jnp.bfloat16).astype(jnp.float32)
                pieces += [high, pk - high]
            firsts[t] = jnp.concatenate(pieces, axis=0).astype(jnp.bfloat16)

    lane_p = lax.broadcasted_iota(jnp.int32, (rows, width), 1)

    def second(s):
        t = plus(me, mixed(s))
        columns = [fetched[slot_of[q, t]] for q in range(4)]
        right = jnp.concatenate(columns + [jnp.zeros((32, 128), jnp.float32)], axis=0).astype(jnp.bfloat16)
        both = lax.dot_general(
            firsts[t], right, (((1,), (1,)), ((), ())), preferred_element_type=jnp.float32
        )
        value = jnp.zeros((rows, width), jnp.float32)
        for q in range(4):
            mine = both[2 * q * rows : (2 * q + 1) * rows] + both[(2 * q + 1) * rows : (2 * q + 2) * rows]
            value = jnp.where((lane_p >= 24 * q) & (lane_p < 24 * (q + 1)), mine, value)
        top = jnp.maximum(jnp.max(jnp.abs(value), axis=1, keepdims=True), FLOOR)
        step = jnp.ceil(jnp.log2(top) * STEPS)
        coded = jnp.round(value * (jnp.exp2(step * (-1.0 / STEPS)) * LEVELS))
        coded = jnp.where(lane_p >= 96, step, coded)
        payload[t] = coded.astype(jnp.int32).astype(jnp.int16)

    def pipelined(make, post):
        @pl.loop(0, LAG)
        def _(g):
            for j in range(4):
                make(4 * g + j + 1)

        @pl.loop(LAG, DEVICES // 4)
        def _(g):
            for j in range(4):
                make(4 * g + j + 1)
            for j in range(4):
                post(4 * (g - LAG) + j + 1)

        @pl.loop(4 * (DEVICES // 4 - LAG) + 1, DEVICES)
        def _(s):
            post(s)

    pipelined(
        second,
        lambda s: push(
            payload, partial_in, plus(me, mixed(s)), send.at[2], recv_row.at[(s - 1) >> 3]
        ),
    )
    keep(payload, partial_in, recv_row.at[DEVICES // GROUP - 1])

    lanes = [lax.broadcasted_iota(jnp.int32, (rows, 128), 1) + 128 * j for j in range(cols // 128)]
    column = [l // 24 for l in lanes]
    within = [l % 24 for l in lanes]
    blocks = cols // 128

    def place(d):
        got = partial_in[d].astype(jnp.int32).astype(jnp.float32)
        value = got * (jnp.exp2(got[:, 96:97] * (1.0 / STEPS)) * (1.0 / LEVELS))
        for j in range(blocks):
            index = jnp.zeros((rows, 128), jnp.int32)
            hit = jnp.zeros((rows, 128), jnp.bool_)
            for q in range(4):
                eq = column[j] == table_s[q + 1, d]
                index = jnp.where(eq, within[j] + 24 * q, index)
                hit = hit | eq
            moved = jnp.take_along_axis(value, index, axis=1)
            spread[d, :, 128 * j : 128 * (j + 1)] = jnp.where(hit, moved, 0.0)

    @pl.loop(0, DEVICES // GROUP)
    def _(g):
        wait_rows(partial_in, GROUP, recv_row.at[g])

        for u in range(GROUP):
            place(minus(me, mixed(g * GROUP + u + 1)))

    plan_copy.wait()

    def add(g, carry):
        terms = [spread[plan_s[0, 4 * g + u]] for u in range(4)]
        for u in range(4):
            joined = plan_s[1, 4 * g + u].astype(jnp.float32)
            carry = carry * joined + terms[u]
            running[4 * g + u] = carry
        return carry

    lax.fori_loop(0, DEVICES // 4, add, jnp.zeros((rows, cols), jnp.float32))

    diagonal = lax.broadcasted_iota(jnp.int32, (rows, 128), 1) == lax.broadcasted_iota(
        jnp.int32, (rows, 128), 0
    )

    def encode(s):
        t = plus(me, mixed(s))
        value = running[plan_s[2, t]] * plan_s[3, t].astype(jnp.float32)
        top = jnp.maximum(jnp.max(jnp.abs(value), axis=1, keepdims=True), FLOOR)
        outgoing[t] = jnp.round(value * (LEVELS / top)).astype(jnp.int32).astype(jnp.int16)
        outscale[t] = jnp.sum(jnp.where(diagonal, top * (1.0 / LEVELS), 0.0), axis=0, keepdims=True)

    def post(s):
        t = plus(me, mixed(s))
        push(outscale, scales, t, send.at[4], recv_scale.at[(s - 1) >> 3])
        push(outgoing, arrived, t, send.at[3], recv_last.at[(s - 1) >> 3])

    pipelined(encode, post)
    keep(outscale, scales, recv_scale.at[DEVICES // GROUP - 1])
    keep(outgoing, arrived, recv_last.at[DEVICES // GROUP - 1])

    @pl.loop(0, DEVICES // GROUP)
    def _(g):
        wait_rows(scales, GROUP, recv_scale.at[g])
        wait_rows(arrived, GROUP, recv_last.at[g])

        for u in range(GROUP):
            t = minus(me, mixed(g * GROUP + u + 1))
            scale = jnp.sum(jnp.where(diagonal, scales[t], 0.0), axis=1, keepdims=True)
            result[t] = arrived[t].astype(jnp.int32).astype(jnp.float32) * scale

    for k, ref in enumerate((ask, stage, payload, outgoing, outscale)):
        wait_rows(ref, others, send.at[k])


def store_kernel(values, out, sem):
    copies = [
        pltpu.make_async_copy(
            values.at[pl.ds(c * GROUP, GROUP)], out.at[pl.ds(c * GROUP, GROUP)], sem.at[c]
        )
        for c in range(DEVICES // GROUP)
    ]
    for copy in copies:
        copy.start()
    for copy in copies:
        copy.wait()


def per_device(prolong, stiffness, request, col_slot, col_pos, coarse_owner):
    slots, per_row, dof, _ = stiffness.shape
    vectors = prolong.shape[1]
    cols = 16 * vectors
    vmem = pl.BlockSpec(memory_space=pltpu.VMEM)
    hbm = pl.BlockSpec(memory_space=pl.ANY)
    result = pl.pallas_call(
        exchange_kernel,
        out_shape=pltpu.VMEM((slots, vectors, cols), jnp.float32),
        in_specs=[hbm] * 6,
        out_specs=vmem,
        scratch_shapes=[
            pltpu.SMEM((slots,), jnp.int32),
            pltpu.SMEM((per_row, slots), jnp.int32),
            pltpu.SMEM((per_row, slots), jnp.int32),
            pltpu.VMEM((1, coarse_owner.shape[0]), jnp.int32),
            pltpu.VMEM(prolong.shape, jnp.bfloat16),
            pltpu.VMEM((slots, per_row, dof, dof), jnp.bfloat16),
            pltpu.VMEM((slots, 1, 128), jnp.int32),
            pltpu.VMEM((slots, 1, 128), jnp.int32),
            pltpu.VMEM((8, 128), jnp.int32),
            pltpu.SMEM((8, 128), jnp.int32),
            pltpu.VMEM((slots, vectors, dof), jnp.bfloat16),
            pltpu.VMEM((slots, vectors, dof), jnp.bfloat16),
            pltpu.VMEM((slots, vectors, dof), jnp.float32),
            pltpu.VMEM((slots, 2 * per_row * vectors, dof), jnp.bfloat16),
            pltpu.VMEM((slots, vectors, 128), jnp.int16),
            pltpu.VMEM((slots, vectors, 128), jnp.int16),
            pltpu.VMEM((8, 128), jnp.int32),
            pltpu.SMEM((8, 128), jnp.int32),
            pltpu.VMEM((slots, vectors, cols), jnp.float32),
            pltpu.VMEM((slots, vectors, cols), jnp.float32),
            pltpu.VMEM((slots, vectors, cols), jnp.int16),
            pltpu.VMEM((slots, vectors, cols), jnp.int16),
            pltpu.VMEM((slots, 1, 128), jnp.float32),
            pltpu.VMEM((slots, 1, 128), jnp.float32),
            pltpu.SemaphoreType.DMA,
            pltpu.SemaphoreType.DMA((5,)),
            pltpu.SemaphoreType.DMA((2,)),
            pltpu.SemaphoreType.DMA((5,)),
            pltpu.SemaphoreType.DMA((1,)),
            pltpu.SemaphoreType.DMA((slots // GROUP,)),
            pltpu.SemaphoreType.DMA((slots // GROUP,)),
            pltpu.SemaphoreType.DMA((slots // GROUP,)),
            pltpu.SemaphoreType.DMA((slots // GROUP,)),
        ],
        compiler_params=pltpu.CompilerParams(
            collective_id=0, has_side_effects=True, vmem_limit_bytes=56 * 1024 * 1024
        ),
        name="galerkin_exchange",
    )(request, col_slot.T, col_pos.T, coarse_owner.T, prolong, stiffness)
    return pl.pallas_call(
        store_kernel,
        out_shape=jax.ShapeDtypeStruct((slots, vectors, cols), jnp.float32),
        in_specs=[vmem],
        out_specs=hbm,
        scratch_shapes=[pltpu.SemaphoreType.DMA((slots // GROUP,))],
        compiler_params=pltpu.CompilerParams(vmem_limit_bytes=16 * 1024 * 1024),
        name="store",
    )(result)


def solution(mesh):
    placed = (
        P(("gx", "gy"), None, None),
        P(("gx", "gy"), None, None, None),
        P(("gx", "gy")),
        P(("gx", "gy"), None),
        P(("gx", "gy"), None),
        P(("gx", "gy"), None),
    )
    return jax.shard_map(
        per_device,
        mesh=mesh,
        in_specs=placed,
        out_specs=P(("gx", "gy"), None, None),
        check_vma=False,
    )
```
